512 devices in a mesh: grp: 2 (over y), tm: 64 (over z, core), space: 4 (over x).
Axes of the slice: x: 4, y: 2, z: 32, core: 2. Of those that a mesh axis runs over, the one named last changes fastest.
The devices are a block of a 4x8x32 slice.
Arguments:
- forcing: float32 [512, 32, 8, 128], P(('grp', 'tm'), 'space'), parts along dimension 0, may hold values from -6 to 6
- start_field: float32 [64, 8, 128], P(('grp', 'space')), parts along dimension 0, may hold values from -6 to 6
- velocity: float32 [3, 32, 8, 128], P(None, 'space'), may hold values from -0.5 to 0.5
- diffusivity: float32 [2], P('grp'), parts along dimension 0, may hold values from 0.3 to 1
Outputs:
- iterate: float32 [512, 32, 8, 128], P(('grp', 'tm'), 'space'), parts along dimension 0
The draws below stay inside these ranges and needn't reach their ends.
There are 2 independent parts, one for each index of `grp`. The reference program is written for one: setup_inputs(seed, part) draws one part's arguments, and reference() takes and returns one part's arrays. A program takes and returns all parts, laid end to end along the dimension named above; an argument that names none is the same for every part. Nothing has to cross between parts.
All inputs are finite; a program needn't handle non-finite values.
Results may differ from the reference program's by a relative error of at most 0.0001.
Values sent between devices are 32-bit elements; how exact they have to be, the bound alone decides.
No kernel may reach another device: no remote copies, remote signals or barrier semaphores. Data moves between devices by JAX's collectives and lax.ppermute only.
A program may use at most 64 MiB of HBM per device.

```python
import math
import jax
import jax.numpy as jnp

NX = 8
NY = 128
SWEEPS = 4
CYCLES = 1
NT = 256
NZ = 32


def levels(key, dims, pieces, smallest, top_value):
    level = 1.0
    for position, blocks in pieces:
        draws = jax.random.uniform(jax.random.fold_in(jax.random.fold_in(key, 6), position), (blocks,), jnp.float32, smallest / len(pieces), top_value / len(pieces))
        level = level * jnp.repeat(jnp.exp(draws), dims[position] // blocks).reshape((-1,) + (1,) * (len(dims) - 1 - position))
    return level


def centred(own_key, extent, spread, limit, cuts=(), held_as=jnp.bfloat16):
    gain = levels(own_key, extent, cuts, -0.22, 0.18) if cuts else 1.0
    drawn = jax.random.normal(own_key, extent, jnp.float32) * spread * gain
    return jnp.minimum(jnp.maximum(drawn, -limit), limit).astype(held_as)


def setup_inputs(seed: int = 0, part: int = 0) -> dict:
    arg_keys = jax.random.split(jax.random.key(seed), 5)
    part_splits = jax.random.split(jax.random.fold_in(arg_keys[4], part), 5)
    return {
        "forcing": centred(part_splits[0], (NT, NZ, NX, NY), 1.0, 6.0, ((0, 64), (1, 4)), jnp.float32),
        "start_field": centred(part_splits[1], (NZ, NX, NY), 1.0, 6.0, ((0, 4),), jnp.float32),
        "velocity": jnp.clip(jax.random.uniform(arg_keys[2], (3, NZ, NX, NY), jnp.float32, -0.5, 0.5) * levels(arg_keys[2], (3, NZ, NX, NY), ((1, 4),), -0.4, 0.0), -0.5, 0.5),
        "diffusivity": jnp.clip(jnp.exp(jax.random.uniform(part_splits[3], (1,), jnp.float32, math.log(0.3), math.log(1.0))), 0.3, 1.0),
    }


time_unit = 0.5


def neighbour_sum(padded, velocity, kappa_value):
    middle = padded[..., 1:-1, :, :]
    higher = padded[..., 2:, :, :]
    beneath = padded[..., :-2, :, :]
    east_side = jnp.roll(middle, -1, axis=-2)
    west_side = jnp.roll(middle, 1, axis=-2)
    north_side = jnp.roll(middle, -1, axis=-1)
    south_side = jnp.roll(middle, 1, axis=-1)
    diffused = kappa_value * (higher + beneath + east_side + west_side + north_side + south_side)
    carried = velocity[0] * (higher - beneath) + velocity[1] * (east_side - west_side) + velocity[2] * (north_side - south_side)
    return diffused - 0.5 * carried


def propagate(source, velocity, kappa_value, time_step):
    diagonal = 1.0 + 6.0 * time_step * kappa_value
    widths = [(0, 0)] * (source.ndim - 3) + [(1, 1), (0, 0), (0, 0)]
    values = source
    for repeat in range(SWEEPS):
        padded = jnp.pad(values, widths)
        values = (source + time_step * neighbour_sum(padded, velocity, kappa_value)) / diagonal
    return values


def relax_points(iterate, forcing, start, velocity, kappa_value, time_step):
    blocks = iterate.shape[0] // 4
    carried = jnp.concatenate([start[None], iterate[3::4][:blocks - 1]], axis=0)
    first_point = propagate(carried, velocity, kappa_value, time_step) + forcing[0::4]
    second_point = propagate(first_point, velocity, kappa_value, time_step) + forcing[1::4]
    third_point = propagate(second_point, velocity, kappa_value, time_step) + forcing[2::4]
    stacked = jnp.stack([first_point, second_point, third_point, iterate[3::4]], axis=1)
    return stacked.reshape(iterate.shape)


def solve_level(level_index, iterate, forcing, start, velocity, kappa_value):
    time_step = time_unit * 4.0 ** level_index
    if iterate.shape[0] == 4:
        previous = start
        points = []
        for offset in range(4):
            previous = propagate(previous, velocity, kappa_value, time_step) + forcing[offset]
            points.append(previous)
        return jnp.stack(points)
    iterate = relax_points(iterate, forcing, start, velocity, kappa_value, time_step)
    if level_index == 0:
        coarse_points = propagate(iterate[2::4], velocity, kappa_value, time_step) + forcing[3::4]
        iterate = iterate.at[3::4].set(coarse_points)
        iterate = relax_points(iterate, forcing, start, velocity, kappa_value, time_step)
    residual = forcing[3::4] + propagate(iterate[2::4], velocity, kappa_value, time_step) - iterate[3::4]
    correction = solve_level(level_index + 1, jnp.zeros_like(residual), residual, jnp.zeros_like(start), velocity, kappa_value)
    iterate = iterate.at[3::4].add(correction)
    return relax_points(iterate, forcing, start, velocity, kappa_value, time_step)


def reference(forcing, start_field, velocity, diffusivity):
    kappa_value = diffusivity[0]
    iterate = jnp.zeros_like(forcing)
    for repeat in range(CYCLES):
        iterate = solve_level(0, iterate, forcing, start_field, velocity, kappa_value)
    return iterate
```

```python
import jax
import jax.numpy as jnp
from jax import lax
from jax.experimental import pallas as pl
from jax.experimental.pallas import tpu as pltpu
from jax.sharding import PartitionSpec as P

SWEEPS = 4
FACTOR = 4
RUN = 2 * FACTOR
TIME_UNIT = 0.5
LEVELS = 4
VMEM = pl.BlockSpec(memory_space=pltpu.VMEM)
SMEM = pl.BlockSpec(memory_space=pltpu.SMEM)
HBM_F32 = jnp.float32


def field(*lead):
    return jax.ShapeDtypeStruct(lead + (8, 128), jnp.float32)


def phi(get, put, coef, ab, level):
    rows = coef.shape[1]
    a, b = ab[level, 0], ab[level, 1]
    v = [get(r) for r in range(rows)]
    base = None
    for sweep in range(SWEEPS):
        new = []
        for r in range(rows):
            x = v[r]
            t = coef[2, r] * pltpu.roll(x, x.shape[0] - 1, 0) + coef[3, r] * pltpu.roll(x, 1, 0)
            t = t + (coef[4, r] * pltpu.roll(x, x.shape[1] - 1, 1) + coef[5, r] * pltpu.roll(x, 1, 1))
            if r + 1 < rows:
                t = t + coef[0, r] * v[r + 1]
            if r > 0:
                t = t + coef[1, r] * v[r - 1]
            new.append(a * get(r) + b * t)
        v = new
    for r in range(rows):
        put(r, v[r])


def fill_coefficients(coef, ab, velocity_row, kappa):
    rows = coef.shape[1]
    k = jnp.full(coef.shape[2:], kappa, jnp.float32)
    for r in range(rows):
        for axis in range(3):
            half = 0.5 * velocity_row(axis, r)
            coef[2 * axis, r] = k - half
            coef[2 * axis + 1, r] = k + half
    for level in range(LEVELS):
        h = TIME_UNIT * float(FACTOR) ** level
        a = 1.0 / (1.0 + (6.0 * h) * k)
        ab[level, 0] = a
        ab[level, 1] = h * a


def place():
    count = lax.axis_size("tm")
    rank = lax.axis_index("tm")
    shifted = (rank + 1) % count
    return count // RUN, rank, shifted // RUN, shifted % RUN


def spread_kernel(kappa, gathered, send, kept, coef, ab, fields):
    runs, rank, run, member = place()
    slab = lax.axis_index("space")
    slabs, chunk = gathered.shape[:2]
    rows_slab = chunk // 8
    rows = slabs * rows_slab
    points = 4

    def row(item, r):
        return gathered[r // rows_slab, item * rows_slab + r % rows_slab]

    fill_coefficients(coef, ab, lambda axis, r: row(points + axis, r), kappa[0])
    first = (rank == 0).astype(jnp.float32)
    ZERO, FORCE, START = 0, 1, 5
    RHO = START + 8
    for r in range(rows):
        fields[ZERO, r] = jnp.zeros(fields.shape[2:], jnp.float32)
        fields[START, r] = row(points + 3, r) * first
        for i in range(points):
            fields[FORCE + i, r] = row(i, r)

    def step(src, dst, level, add):
        phi(
            lambda r: fields[src, r],
            lambda r, value: fields.__setitem__((dst, r), value + fields[add, r]),
            coef, ab, level,
        )

    Y = RHO + 7
    Z1, Z2 = Y + 1, Y + 2
    E1 = Z2 + 1
    H = E1 + 3
    power = RHO + (FACTOR - 1 - member) % FACTOR
    y = jnp.where(member < FACTOR, Y, power)
    odd = run % 2 == 0
    z = jnp.where(odd, Z2, y)

    def body(n, carry):
        main = n < 14
        m = n - 14
        src = jnp.where(m == 0, power, jnp.where(m == 1, y, jnp.where(m == 3, z, Y + m - 1)))
        pair = (m - 6) // 2
        hsrc = jnp.where(m % 2 == 0, jnp.where(pair == 0, z, E1 + pair - 1), Y + m - 1)
        src = jnp.where(m >= 6, hsrc, src)
        src = jnp.where(main, START + n, src)
        dst = jnp.where(main, START + n + 1, Y + m)
        level = jnp.where(main, jnp.where(n < 8, 0, 1), jnp.where((m >= 3) & (m < 6), 3, 2))
        add = jnp.where(n < points, FORCE + n, ZERO)
        step(src, dst, level, add)
        return carry

    lax.fori_loop(0, 26, body, 0)

    def store(target, source):
        for j in range(RUN):
            send[j, target] = fields[source, slab * rows_slab + j]

    valid = (run > 0) | (member > 0)
    this_run = run + 1
    level2 = run // 2 + 1
    for target in range(RUN):
        goal = target + 1 if target else RUN + 1
        if goal % 2 == 1:
            k = (goal + 1) // 2 - 1 - level2
            source = jnp.where(k == 0, z, E1 + k - 1)
            use = k >= 0
        else:
            k = goal // 2 - 1 - level2
            source = jnp.where(k < 0, y, H + 2 * k + 1)
            use = goal > this_run
        source = jnp.where(valid & use, source, ZERO)
        store(target, source)
    for j in range(RUN):
        source = jnp.where((j > member) & valid, RHO + jnp.maximum(j - member - 1, 0), ZERO)
        source = jnp.where(j == member, START + 4, source)
        store(RUN + j, source)
    for i in range(points - 1):
        for r in range(rows_slab):
            kept[i, r] = fields[START + 1 + i, slab * rows_slab + r]


def sum_kernel(received, targets, prefixes):
    for t in range(RUN):
        total, prefix = received[0, t], received[0, RUN + t]
        for j in range(1, received.shape[0]):
            total = total + received[j, t]
            prefix = prefix + received[j, RUN + t]
        targets[t] = total
        prefixes[t] = prefix


def share_kernel(received, prefixes, send):
    total = received[0]
    for j in range(1, received.shape[0]):
        total = total + received[j]
    for j in range(RUN):
        own = prefixes[j]
        before = prefixes[max(j - 1, 0)]
        for s in range(send.shape[1]):
            send[j, s, 0] = total
            send[j, s, 1] = own
            send[j, s, 2] = before


def boundary_kernel(received, coef, ab, after, before, v):
    runs, rank, run, member = place()
    rows = coef.shape[1]
    slabs = received.shape[1]
    rows_slab = rows // slabs
    real = jnp.where((run > 0) | (member == 0), 1.0, 0.0)

    def item(which, r):
        return received[r % rows_slab, r // rows_slab, which]

    for r in range(rows):
        v[r] = item(0, r) * real
    ones = member % FACTOR
    odd = member % 2
    twos = member // FACTOR

    def body(n, carry):
        phi(lambda r: v[r], lambda r, value: v.__setitem__(r, value), coef, ab, jnp.where(n < twos, 2, 1))
        return carry

    lax.fori_loop(0, twos + ones - odd, body, 0)
    keep = jnp.where(rank == 0, 0.0, 1.0)
    for r in range(rows):
        before[r] = (item(2, r) + v[r]) * keep
    lax.fori_loop(twos + ones - odd, twos + ones, body, 0)
    for r in range(rows):
        after[r] = item(1, r) + v[r]


def final_kernel(passed, before, after, kept, coef, ab, out, v):
    runs, rank, run, member = place()
    slab = lax.axis_index("space")
    rows = coef.shape[1]
    rows_slab = out.shape[1]
    partner = member % 2 == 0
    for r in range(rows):
        v[r] = jnp.where(partner, passed[r], before[r])
    for i in range(3):
        phi(lambda r: v[r], lambda r, value: v.__setitem__(r, value), coef, ab, 0)
        for r in range(rows_slab):
            out[i, r] = kept[i, r] + v[slab * rows_slab + r]
    for r in range(rows_slab):
        out[3, r] = after[slab * rows_slab + r]


def call(kernel, inputs, outputs, scratch=(), smem=()):
    return pl.pallas_call(
        kernel,
        out_shape=outputs,
        in_specs=[SMEM if i in smem else VMEM for i in range(len(inputs))],
        out_specs=jax.tree.map(lambda _: VMEM, outputs),
        scratch_shapes=[pltpu.VMEM(s, jnp.float32) for s in scratch],
    )(*inputs)


def local(forcing, start_field, velocity, diffusivity):
    count = lax.axis_size("tm")
    slabs = lax.axis_size("space")
    runs = count // RUN
    rows_slab = forcing.shape[1]
    rows = rows_slab * slabs
    tile = forcing.shape[2:]

    near = [[(RUN * g + j - 1) % count for j in range(RUN)] for g in range(runs)]
    far = [[(RUN * g + j - 1) % count for g in range(runs)] for j in range(RUN)]
    wide = [[q * slabs + s for q in group for s in range(slabs)] for group in near]

    own = jnp.concatenate([forcing, velocity, start_field[None]], axis=0)
    own = own.reshape((1, 8 * rows_slab) + tile)
    gathered = lax.all_to_all(
        jnp.broadcast_to(own, (slabs,) + own.shape[1:]), "space", 0, 0, tiled=True
    )
    send, kept, coef, ab = call(
        spread_kernel,
        (diffusivity, gathered),
        (field(RUN, 2 * RUN), field(3, rows_slab), field(6, rows), field(LEVELS, 2)),
        scratch=[(32, rows) + tile],
        smem=(0,),
    )
    received = lax.all_to_all(send, "tm", 0, 0, axis_index_groups=near, tiled=True)
    targets, prefixes = call(sum_kernel, (received,), (field(RUN), field(RUN)))
    received = lax.all_to_all(targets, "tm", 0, 0, axis_index_groups=far, tiled=True)
    send = call(share_kernel, (received, prefixes), field(RUN, slabs, 3))
    send = send.reshape((RUN * slabs, 3) + tile)
    received = lax.all_to_all(send, ("tm", "space"), 0, 0, axis_index_groups=wide, tiled=True)
    received = received.reshape((RUN, slabs, 3) + tile)
    after, before = call(
        boundary_kernel, (received, coef, ab), (field(rows), field(rows)), scratch=[(rows,) + tile]
    )
    passed = lax.ppermute(after, "tm", [(q, q + 1) for q in range(0, count, 2)])
    return call(
        final_kernel,
        (passed, before, after, kept, coef, ab),
        field(4, rows_slab),
        scratch=[(rows,) + tile],
    )


def solution(mesh):
    if mesh.shape["tm"] != FACTOR**3:
        raise ValueError("time axis")
    placed = (
        P(("grp", "tm"), "space", None, None),
        P(("grp", "space"), None, None),
        P(None, "space", None, None),
        P("grp"),
    )
    return jax.shard_map(
        local,
        mesh=mesh,
        in_specs=placed,
        out_specs=P(("grp", "tm"), "space", None, None),
        check_vma=False,
    )
```

```python
import jax
import jax.numpy as jnp
from jax import lax
from jax.experimental import pallas as pl
from jax.experimental.pallas import tpu as pltpu
from jax.sharding import PartitionSpec as P

SWEEPS = 4
FACTOR = 4
RUN = 2 * FACTOR
TIME_UNIT = 0.5
LEVELS = 4
VMEM = pl.BlockSpec(memory_space=pltpu.VMEM)
SMEM = pl.BlockSpec(memory_space=pltpu.SMEM)


def field(*lead):
    return jax.ShapeDtypeStruct(lead + (8, 128), jnp.float32)


def phi(get, put, coef, ab, level):
    rows = coef.shape[1]
    a, b = ab[level, 0], ab[level, 1]
    v = [get(r) for r in range(rows)]
    base = None
    for sweep in range(SWEEPS):
        new = []
        for r in range(rows):
            x = v[r]
            t = coef[2, r] * pltpu.roll(x, x.shape[0] - 1, 0) + coef[3, r] * pltpu.roll(x, 1, 0)
            t = t + (coef[4, r] * pltpu.roll(x, x.shape[1] - 1, 1) + coef[5, r] * pltpu.roll(x, 1, 1))
            if r + 1 < rows:
                t = t + coef[0, r] * v[r + 1]
            if r > 0:
                t = t + coef[1, r] * v[r - 1]
            new.append(a * get(r) + b * t)
        v = new
    for r in range(rows):
        put(r, v[r])


def fill_coefficients(coef, ab, velocity_row, kappa):
    rows = coef.shape[1]
    k = jnp.full(coef.shape[2:], kappa, jnp.float32)
    for r in range(rows):
        for axis in range(3):
            half = 0.5 * velocity_row(axis, r)
            coef[2 * axis, r] = k - half
            coef[2 * axis + 1, r] = k + half
    for level in range(LEVELS):
        h = TIME_UNIT * float(FACTOR) ** level
        a = 1.0 / (1.0 + (6.0 * h) * k)
        ab[level, 0] = a
        ab[level, 1] = h * a


def place():
    rank = lax.axis_index("tm")
    return rank // RUN, rank % RUN


def chain_kernel(kappa, gathered, last, kept, coef, ab, fields):
    slab = lax.axis_index("space")
    slabs, chunk = gathered.shape[:2]
    rows_slab = chunk // 8
    rows = slabs * rows_slab
    points = 4

    def row(item, r):
        return gathered[r // rows_slab, item * rows_slab + r % rows_slab]

    fill_coefficients(coef, ab, lambda axis, r: row(points + axis, r), kappa[0])
    first = (lax.axis_index("tm") == 0).astype(jnp.float32)
    for r in range(rows):
        fields[0, r] = row(points + 3, r) * first

    def body(n, carry):
        phi(
            lambda r: fields[n, r],
            lambda r, value: fields.__setitem__((n + 1, r), value + row(n, r)),
            coef, ab, 0,
        )
        return carry

    lax.fori_loop(0, points, body, 0)
    for r in range(rows):
        last[r] = fields[points, r]
    for i in range(points):
        for r in range(rows_slab):
            kept[i, r] = fields[1 + i, slab * rows_slab + r]


def spread_kernel(before, kept, coef, ab, send, held, fields):
    run, member = place()
    slab = lax.axis_index("space")
    rows = coef.shape[1]
    rows_slab = kept.shape[1]
    RHO = 4
    Y = RHO + 7
    Z2 = Y + 2
    E1 = Z2 + 1
    H = E1 + 3
    ZERO = fields.shape[0] - 1
    for r in range(rows):
        fields[0, r] = before[r]
    for j in range(rows_slab):
        fields[ZERO, slab * rows_slab + j] = jnp.zeros(fields.shape[2:], jnp.float32)
    power = RHO + (FACTOR - 1 - member) % FACTOR
    y = jnp.where(member < FACTOR, Y, power)
    z = jnp.where(run % 2 == 0, Z2, y)

    def body(n, carry):
        m = n - 10
        src = jnp.where(m == 0, power, jnp.where(m == 1, y, jnp.where(m == 3, z, Y + m - 1)))
        pair = (m - 6) // 2
        hsrc = jnp.where(m % 2 == 0, jnp.where(pair == 0, z, E1 + pair - 1), Y + m - 1)
        src = jnp.where(m >= 6, hsrc, src)
        src = jnp.where(m < 0, n, src)
        dst = jnp.where(m < 0, n + 1, Y + m)
        level = jnp.where(m < 0, jnp.where(n < 4, 0, 1), jnp.where((m >= 3) & (m < 6), 3, 2))
        phi(
            lambda r: fields[src, r],
            lambda r, value: fields.__setitem__((dst, r), value),
            coef, ab, level,
        )
        return carry

    lax.fori_loop(0, 22, body, 0)

    def store(slot, source):
        for j in range(RUN):
            send[j, slot] = fields[source, slab * rows_slab + j]

    level2 = run // 2 + 1
    for slot in range(RUN):
        goal = slot + 2
        if goal % 2 == 1:
            k = (goal + 1) // 2 - 1 - level2
            source = jnp.where(k == 0, z, E1 + k - 1)
            use = k >= 0
        else:
            k = goal // 2 - 1 - level2
            source = jnp.where(k < 0, y, H + 2 * k + 1)
            use = goal > run + 1
        store(slot, jnp.where(use, source, ZERO))
    for j in range(1, RUN):
        store(RUN + j - 1, jnp.where(j > member, RHO + jnp.maximum(j - member - 1, 0), ZERO))
    for r in range(rows_slab):
        for i in range(3):
            held[i, r] = kept[i, r] + fields[1 + i, slab * rows_slab + r]
        held[3, r] = kept[3, r]
        held[4, r] = fields[RHO, slab * rows_slab + r]


def sum_kernel(received, goals, prefixes):
    for t in range(2 * RUN - 1):
        total = received[0, t]
        for j in range(1, received.shape[0]):
            total = total + received[j, t]
        if t < RUN:
            goals[t] = total
        else:
            prefixes[t - RUN] = total


def share_kernel(goals, prefixes, send):
    run, _ = place()
    tile = goals.shape[1:]
    entry = jnp.where(run > 0, 1.0, 0.0) * goals[jnp.maximum(run - 1, 0)]
    leave = goals[run]
    for j in range(RUN):
        prefix = prefixes[j - 1] if j else jnp.zeros(tile, jnp.float32)
        extra = leave if j == RUN - 1 else prefixes[FACTOR - 1]
        for s in range(send.shape[1]):
            send[j, s, 0] = entry
            send[j, s, 1] = prefix
            send[j, s, 2] = extra


def final_kernel(received, held, coef, ab, out, v):
    run, member = place()
    slab = lax.axis_index("space")
    rows = coef.shape[1]
    rows_slab = out.shape[1]

    def item(which, r):
        return received[r % rows_slab, r // rows_slab, which]

    for r in range(rows):
        v[0, r] = item(0, r)
        v[1, r] = item(0, r)
    ones = member % FACTOR
    twos = member // FACTOR

    def apply(dst, src, level):
        phi(lambda r: v[src, r], lambda r, value: v.__setitem__((dst, r), value), coef, ab, level)

    def body(n, carry):
        apply(1, 1, jnp.where(n < twos, 2, 1))
        return carry

    lax.fori_loop(0, twos + ones, body, 0)
    for r in range(rows):
        v[1, r] = v[1, r] + item(1, r)
    middle = member == FACTOR - 1
    apply(2, jnp.where(middle, 0, 1), jnp.where(middle, 2, 1))
    end = member == RUN - 1
    for r in range(rows_slab):
        extra = received[r, slab, 2]
        added = jnp.where(middle, extra, held[4, r])
        moved = jnp.where(end, extra, v[2, slab * rows_slab + r] + added)
        out[3, r] = held[3, r] + moved

    def last(i, carry):
        apply(1, 1, 0)
        for r in range(rows_slab):
            out[i, r] = held[i, r] + v[1, slab * rows_slab + r]
        return carry

    lax.fori_loop(0, 3, last, 0)


def call(kernel, inputs, outputs, scratch=(), smem=(), mib=4):
    return pl.pallas_call(
        kernel,
        out_shape=outputs,
        in_specs=[SMEM if i in smem else VMEM for i in range(len(inputs))],
        out_specs=jax.tree.map(lambda _: VMEM, outputs),
        scratch_shapes=[pltpu.VMEM(s, jnp.float32) for s in scratch],
        compiler_params=pltpu.CompilerParams(vmem_limit_bytes=mib << 20),
    )(*inputs)


def local(forcing, start_field, velocity, diffusivity):
    count = lax.axis_size("tm")
    slabs = lax.axis_size("space")
    runs = count // RUN
    rows_slab = forcing.shape[1]
    rows = rows_slab * slabs
    tile = forcing.shape[2:]

    near = [[RUN * g + j for j in range(RUN)] for g in range(runs)]
    wide = [[q * slabs + s for q in group for s in range(slabs)] for group in near]

    own = jnp.concatenate([forcing, velocity, start_field[None]], axis=0)
    own = own.reshape((1, 8 * rows_slab) + tile)
    gathered = lax.all_to_all(
        jnp.broadcast_to(own, (slabs,) + own.shape[1:]), "space", 0, 0, tiled=True
    )
    last, kept, coef, ab = call(
        chain_kernel,
        (diffusivity, gathered),
        (field(rows), field(4, rows_slab), field(6, rows), field(LEVELS, 2)),
        scratch=[(5, rows) + tile],
        smem=(0,),
        mib=6,
    )
    before = lax.ppermute(last, "tm", [(q, q + 1) for q in range(count - 1)])
    send, held = call(
        spread_kernel,
        (before, kept, coef, ab),
        (field(RUN, 2 * RUN - 1), field(5, rows_slab)),
        scratch=[(25, rows) + tile],
        mib=8,
    )
    received = lax.all_to_all(send, "tm", 0, 0, axis_index_groups=near, tiled=True)
    goals, prefixes = call(sum_kernel, (received,), (field(RUN), field(RUN - 1)))
    for g in range(runs - 1):
        goals = goals + lax.ppermute(goals, "tm", list(zip(near[g], near[g + 1])))
    send = call(share_kernel, (goals, prefixes), field(RUN, slabs, 3))
    send = send.reshape((RUN * slabs, 3) + tile)
    received = lax.all_to_all(send, ("tm", "space"), 0, 0, axis_index_groups=wide, tiled=True)
    received = received.reshape((RUN, slabs, 3) + tile)
    return call(
        final_kernel,
        (received, held, coef, ab),
        field(4, rows_slab),
        scratch=[(3, rows) + tile],
    )


def solution(mesh):
    if mesh.shape["tm"] != FACTOR**3:
        raise ValueError("time axis")
    placed = (
        P(("grp", "tm"), "space", None, None),
        P(("grp", "space"), None, None),
        P(None, "space", None, None),
        P("grp"),
    )
    return jax.shard_map(
        local,
        mesh=mesh,
        in_specs=placed,
        out_specs=P(("grp", "tm"), "space", None, None),
        check_vma=False,
    )
```

```python
import jax
import jax.numpy as jnp
from jax import lax
from jax.experimental import pallas as pl
from jax.experimental.pallas import tpu as pltpu
from jax.sharding import PartitionSpec as P

SWEEPS = 4
FACTOR = 4
TIME_UNIT = 0.5
LEVELS = 4
VMEM = pl.BlockSpec(memory_space=pltpu.VMEM)
SMEM = pl.BlockSpec(memory_space=pltpu.SMEM)


def field(*lead):
    return jax.ShapeDtypeStruct(lead + (8, 128), jnp.float32)


def phi(get, put, coef, ab, level):
    rows = coef.shape[1]
    a, b = ab[level, 0], ab[level, 1]
    v = [get(r) for r in range(rows)]
    base = None
    for sweep in range(SWEEPS):
        new = []
        for r in range(rows):
            x = v[r]
            t = coef[2, r] * pltpu.roll(x, x.shape[0] - 1, 0) + coef[3, r] * pltpu.roll(x, 1, 0)
            t = t + (coef[4, r] * pltpu.roll(x, x.shape[1] - 1, 1) + coef[5, r] * pltpu.roll(x, 1, 1))
            if r + 1 < rows:
                t = t + coef[0, r] * v[r + 1]
            if r > 0:
                t = t + coef[1, r] * v[r - 1]
            new.append(a * get(r) + b * t)
        v = new
    for r in range(rows):
        put(r, v[r])


def fill_coefficients(coef, ab, velocity_row, kappa):
    rows = coef.shape[1]
    k = jnp.full(coef.shape[2:], kappa, jnp.float32)
    for r in range(rows):
        for axis in range(3):
            half = 0.5 * velocity_row(axis, r)
            coef[2 * axis, r] = k - half
            coef[2 * axis + 1, r] = k + half
    for level in range(LEVELS):
        h = TIME_UNIT * float(FACTOR) ** level
        a = 1.0 / (1.0 + (6.0 * h) * k)
        ab[level, 0] = a
        ab[level, 1] = h * a


def place():
    rank = lax.axis_index("tm")
    block = rank // FACTOR
    return block // FACTOR, block % FACTOR, rank % FACTOR


def chain_kernel(kappa, gathered, last, kept, coef, ab, fields):
    slab = lax.axis_index("space")
    slabs, chunk = gathered.shape[:2]
    rows_slab = chunk // 8
    rows = slabs * rows_slab
    points = 4

    def row(item, r):
        return gathered[r // rows_slab, item * rows_slab + r % rows_slab]

    fill_coefficients(coef, ab, lambda axis, r: row(points + axis, r), kappa[0])
    first = (lax.axis_index("tm") == 0).astype(jnp.float32)
    for r in range(rows):
        fields[0, r] = row(points + 3, r) * first

    def body(n, carry):
        phi(
            lambda r: fields[n, r],
            lambda r, value: fields.__setitem__((n + 1, r), value + row(n, r)),
            coef, ab, 0,
        )
        return carry

    lax.fori_loop(0, points, body, 0)
    for r in range(rows):
        last[r] = fields[points, r]
    for i in range(points):
        for r in range(rows_slab):
            kept[i, r] = fields[1 + i, slab * rows_slab + r]


def residual_kernel(before, kept, coef, ab, send, held, fields):
    slab = lax.axis_index("space")
    rows = coef.shape[1]
    rows_slab = kept.shape[1]
    for r in range(rows):
        fields[0, r] = before[r]

    def body(n, carry):
        phi(
            lambda r: fields[n, r],
            lambda r, value: fields.__setitem__((n + 1, r), value),
            coef, ab, 0,
        )
        return carry

    lax.fori_loop(0, 4, body, 0)
    for r in range(rows):
        value = fields[4, r]
        for j in range(send.shape[0]):
            send[j, r] = value
    for r in range(rows_slab):
        for i in range(3):
            held[i, r] = kept[i, r] + fields[1 + i, slab * rows_slab + r]
        held[3, r] = kept[3, r]


def spread_kernel(residuals, coef, ab, parts, prefix, added, fields):
    wide, place2, member = place()
    slab = lax.axis_index("space")
    rows = coef.shape[1]
    rows_slab = added.shape[0]
    own = parts.shape[1]
    for r in range(rows):
        fields[0, r] = jnp.zeros(fields.shape[2:], jnp.float32)
        fields[1, r] = residuals[0, r]

    def step(src, dst, level, add):
        phi(
            lambda r: fields[src, r],
            lambda r, value: fields.__setitem__((dst, r), add(r, value)),
            coef, ab, level,
        )

    def sums(n, carry):
        step(n, n + 1, 1, lambda r, value: value + residuals[n, r])
        return carry

    lax.fori_loop(1, FACTOR, sums, 0)
    total = FACTOR
    z = total + FACTOR - 1 - place2

    def powers(n, carry):
        src = jnp.where(n == 7, z, n)
        step(src, n + 1, jnp.where(n < 7, 2, 3), lambda r, value: value)
        return carry

    lax.fori_loop(4, 10, powers, 0)

    def store(slot, source):
        for j in range(own):
            parts[slot, j] = fields[source, slab * rows_slab + member * own + j]

    for later in range(1, FACTOR):
        n = later - 1 - place2
        store(later - 1, jnp.where(n >= 0, total + n, 0))
    for goal in range(FACTOR):
        n = goal - wide
        store(FACTOR - 1 + goal, jnp.where(n < 0, 0, jnp.where(n == 0, z, 7 + n)))
    for r in range(rows):
        prefix[r] = fields[member, r]
    end = member == FACTOR - 1
    for r in range(rows_slab):
        at = slab * rows_slab + r
        added[r] = jnp.where(end, fields[total, at], residuals[member, at])


def share_kernel(parts, entry, handed, send):
    wide, place2, _ = place()
    last = place2 == FACTOR - 1
    inner = jnp.where(place2 > 0, 1.0, 0.0)
    for j in range(parts.shape[1]):
        outer = jnp.where(last, entry[jnp.maximum(wide - 1, 0), j], handed[j])
        level2 = parts[jnp.maximum(place2 - 1, 0), j] * inner
        for a in range(send.shape[0]):
            for s in range(send.shape[1]):
                send[a, s, 0, j] = outer
                send[a, s, 1, j] = level2


def final_kernel(received, prefix, added, held, coef, ab, out, v):
    wide, place2, member = place()
    slab = lax.axis_index("space")
    rows = coef.shape[1]
    rows_slab = out.shape[1]
    own = received.shape[3]

    def item(which, r):
        return received[r % rows_slab // own, r // rows_slab, which, r % own]

    for r in range(rows):
        v[0, r] = item(0, r)
        v[1, r] = item(0, r)
        v[3, r] = item(1, r)

    def apply(dst, src, level):
        phi(lambda r: v[src, r], lambda r, value: v.__setitem__((dst, r), value), coef, ab, level)

    def body(level):
        def run(n, carry):
            apply(1, 1, level)
            return carry

        return run

    lax.fori_loop(0, place2, body(2), 0)
    for r in range(rows):
        entry = v[1, r] + v[3, r]
        v[1, r] = entry
        v[4, r] = entry
    lax.fori_loop(0, member, body(1), 0)
    for r in range(rows):
        v[1, r] = v[1, r] + prefix[r]
        v[5, r] = jnp.zeros(v.shape[2:], jnp.float32)
    end = member == FACTOR - 1
    both = end & (place2 == FACTOR - 1)
    apply(2, jnp.where(both, 0, jnp.where(end, 4, 1)), jnp.where(both, 3, jnp.where(end, 2, 1)))

    def second(n, carry):
        apply(5, 3, 2)
        return carry

    lax.fori_loop(0, jnp.where(both, 1, 0), second, 0)
    for r in range(rows_slab):
        at = slab * rows_slab + r
        out[3, r] = held[3, r] + (v[2, at] + v[5, at] + added[r])

    def last(i, carry):
        apply(1, 1, 0)
        for r in range(rows_slab):
            out[i, r] = held[i, r] + v[1, slab * rows_slab + r]
        return carry

    lax.fori_loop(0, 3, last, 0)


def call(kernel, inputs, outputs, scratch=(), smem=(), mib=4):
    return pl.pallas_call(
        kernel,
        out_shape=outputs,
        in_specs=[SMEM if i in smem else VMEM for i in range(len(inputs))],
        out_specs=jax.tree.map(lambda _: VMEM, outputs),
        scratch_shapes=[pltpu.VMEM(s, jnp.float32) for s in scratch],
        compiler_params=pltpu.CompilerParams(vmem_limit_bytes=mib << 20),
    )(*inputs)


def local(forcing, start_field, velocity, diffusivity):
    count = lax.axis_size("tm")
    slabs = lax.axis_size("space")
    blocks = count // FACTOR
    wides = blocks // FACTOR
    rows_slab = forcing.shape[1]
    rows = rows_slab * slabs
    own_rows = rows_slab // FACTOR
    tile = forcing.shape[2:]

    near = [[FACTOR * m + j for j in range(FACTOR)] for m in range(blocks)]
    square = [[q * slabs + s for q in group for s in range(slabs)] for group in near]

    def hop(value, pairs):
        moves = []
        for source, target in pairs:
            moves += zip(near[source[0] * FACTOR + source[1]], near[target[0] * FACTOR + target[1]])
        return lax.ppermute(value, "tm", moves)

    own = jnp.concatenate([forcing, velocity, start_field[None]], axis=0)
    own = own.reshape((1, 8 * rows_slab) + tile)
    gathered = lax.all_to_all(
        jnp.broadcast_to(own, (slabs,) + own.shape[1:]), "space", 0, 0, tiled=True
    )
    last, kept, coef, ab = call(
        chain_kernel,
        (diffusivity, gathered),
        (field(rows), field(4, rows_slab), field(6, rows), field(LEVELS, 2)),
        scratch=[(5, rows) + tile],
        smem=(0,),
        mib=6,
    )
    before = lax.ppermute(last, "tm", [(q, q + 1) for q in range(count - 1)])
    send, held = call(
        residual_kernel,
        (before, kept, coef, ab),
        (field(FACTOR, rows), field(4, rows_slab)),
        scratch=[(5, rows) + tile],
    )
    residuals = lax.all_to_all(send, "tm", 0, 0, axis_index_groups=near, tiled=True)
    parts, prefix, added = call(
        spread_kernel,
        (residuals, coef, ab),
        (field(2 * FACTOR - 1, own_rows), field(rows), field(rows_slab)),
        scratch=[(11, rows) + tile],
        mib=6,
    )
    ends = FACTOR - 1
    parts = parts + hop(parts, [((w, i), (w, i + 1)) for w in range(wides) for i in (0, 2)])
    to_last = hop(parts, [((w, 1), (w, 3)) for w in range(wides)])
    to_next = hop(parts, [((w, 1), (w, 2)) for w in range(wides)])
    parts = parts + to_last + to_next
    goals = parts[FACTOR - 1 :]
    entry = jnp.zeros_like(goals)
    for w in range(wides - 1):
        entry = entry + hop(goals + entry, [((w, ends), (w + 1, ends))])
    wide = lax.div(lax.axis_index("tm"), count // wides)
    leave = lax.dynamic_slice(goals + entry, (wide, 0, 0, 0), (1,) + goals.shape[1:])[0]
    handed = jnp.zeros_like(leave)
    for i in range(ends):
        handed = handed + hop(leave, [((w, ends), (w + 1, i)) for w in range(wides - 1)])
    send = call(share_kernel, (parts, entry, handed), field(FACTOR, slabs, 2, own_rows))
    send = send.reshape((FACTOR * slabs, 2, own_rows) + tile)
    received = lax.all_to_all(send, ("tm", "space"), 0, 0, axis_index_groups=square, tiled=True)
    received = received.reshape((FACTOR, slabs, 2, own_rows) + tile)
    return call(
        final_kernel,
        (received, prefix, added, held, coef, ab),
        field(4, rows_slab),
        scratch=[(6, rows) + tile],
    )


def solution(mesh):
    if mesh.shape["tm"] != FACTOR**3:
        raise ValueError("time axis")
    placed = (
        P(("grp", "tm"), "space", None, None),
        P(("grp", "space"), None, None),
        P(None, "space", None, None),
        P("grp"),
    )
    return jax.shard_map(
        local,
        mesh=mesh,
        in_specs=placed,
        out_specs=P(("grp", "tm"), "space", None, None),
        check_vma=False,
    )
```

```python
import jax
import jax.numpy as jnp
from jax import lax
from jax.experimental import pallas as pl
from jax.experimental.pallas import tpu as pltpu
from jax.sharding import PartitionSpec as P

SWEEPS = 4
FACTOR = 4
TIME_UNIT = 0.5
LEVELS = 4
VMEM = pl.BlockSpec(memory_space=pltpu.VMEM)
SMEM = pl.BlockSpec(memory_space=pltpu.SMEM)


def field(*lead):
    return jax.ShapeDtypeStruct(lead + (8, 128), jnp.float32)


def phi(get, put, coef, ab, level):
    rows = coef.shape[1]
    a, b = ab[level, 0], ab[level, 1]
    v = [get(r) for r in range(rows)]
    base = None
    for sweep in range(SWEEPS):
        new = []
        for r in range(rows):
            x = v[r]
            t = coef[2, r] * pltpu.roll(x, x.shape[0] - 1, 0) + coef[3, r] * pltpu.roll(x, 1, 0)
            t = t + (coef[4, r] * pltpu.roll(x, x.shape[1] - 1, 1) + coef[5, r] * pltpu.roll(x, 1, 1))
            if r + 1 < rows:
                t = t + coef[0, r] * v[r + 1]
            if r > 0:
                t = t + coef[1, r] * v[r - 1]
            new.append(a * get(r) + b * t)
        v = new
    for r in range(rows):
        put(r, v[r])


def fill_coefficients(coef, ab, velocity_row, kappa):
    rows = coef.shape[1]
    k = jnp.full(coef.shape[2:], kappa, jnp.float32)
    for r in range(rows):
        for axis in range(3):
            half = 0.5 * velocity_row(axis, r)
            coef[2 * axis, r] = k - half
            coef[2 * axis + 1, r] = k + half
    for level in range(LEVELS):
        h = TIME_UNIT * float(FACTOR) ** level
        a = 1.0 / (1.0 + (6.0 * h) * k)
        ab[level, 0] = a
        ab[level, 1] = h * a


def place():
    rank = lax.axis_index("tm")
    block = rank // FACTOR
    return block // FACTOR, block % FACTOR, rank % FACTOR


def lay_out_kernel(forcing, velocity, start, own, done):
    copies = []
    for s in range(own.shape[0]):
        copies += [
            pltpu.make_async_copy(forcing, own.at[s, pl.ds(0, 4)], done.at[s, 0]),
            pltpu.make_async_copy(velocity, own.at[s, pl.ds(4, 3)], done.at[s, 1]),
            pltpu.make_async_copy(start, own.at[s, 7], done.at[s, 2]),
        ]
    for copy in copies:
        copy.start()
    for copy in copies:
        copy.wait()


def chain_kernel(kappa, gathered, last, kept, coef, ab, fields):
    slab = lax.axis_index("space")
    slabs, chunk = gathered.shape[:2]
    rows_slab = chunk // 8
    rows = slabs * rows_slab
    points = 4

    def row(item, r):
        return gathered[r // rows_slab, item * rows_slab + r % rows_slab]

    fill_coefficients(coef, ab, lambda axis, r: row(points + axis, r), kappa[0])
    first = (lax.axis_index("tm") == 0).astype(jnp.float32)
    for r in range(rows):
        fields[0, r] = row(points + 3, r) * first

    def body(n, carry):
        phi(
            lambda r: fields[n, r],
            lambda r, value: fields.__setitem__((n + 1, r), value + row(n, r)),
            coef, ab, 0,
        )
        return carry

    lax.fori_loop(0, points, body, 0)
    for r in range(rows):
        last[r] = fields[points, r]
    for i in range(points):
        for r in range(rows_slab):
            kept[i, r] = fields[1 + i, slab * rows_slab + r]


def residual_kernel(before, kept, coef, ab, send, held, fields):
    slab = lax.axis_index("space")
    rows = coef.shape[1]
    rows_slab = kept.shape[1]
    for r in range(rows):
        fields[0, r] = before[r]

    def body(n, carry):
        phi(
            lambda r: fields[n, r],
            lambda r, value: fields.__setitem__((n + 1, r), value),
            coef, ab, 0,
        )
        return carry

    lax.fori_loop(0, 4, body, 0)
    for r in range(rows):
        value = fields[4, r]
        for j in range(send.shape[0]):
            send[j, r] = value
    for r in range(rows_slab):
        for i in range(3):
            held[i, r] = kept[i, r] + fields[1 + i, slab * rows_slab + r]
        held[3, r] = kept[3, r]


def spread_kernel(residuals, coef, ab, parts, prefix, added, fields):
    wide, place2, member = place()
    slab = lax.axis_index("space")
    rows = coef.shape[1]
    rows_slab = added.shape[0]
    own = parts.shape[1]
    for r in range(rows):
        fields[0, r] = jnp.zeros(fields.shape[2:], jnp.float32)
        fields[1, r] = residuals[0, r]

    def step(src, dst, level, add):
        phi(
            lambda r: fields[src, r],
            lambda r, value: fields.__setitem__((dst, r), add(r, value)),
            coef, ab, level,
        )

    def sums(n, carry):
        step(n, n + 1, 1, lambda r, value: value + residuals[n, r])
        return carry

    lax.fori_loop(1, FACTOR, sums, 0)
    total = FACTOR
    z = total + FACTOR - 1 - place2

    def powers(n, carry):
        src = jnp.where(n == 7, z, n)
        step(src, n + 1, jnp.where(n < 7, 2, 3), lambda r, value: value)
        return carry

    lax.fori_loop(4, 10, powers, 0)

    def store(slot, source):
        for j in range(own):
            parts[slot, j] = fields[source, slab * rows_slab + member * own + j]

    for later in range(1, FACTOR):
        n = later - 1 - place2
        store(later - 1, jnp.where(n >= 0, total + n, 0))
    for goal in range(FACTOR):
        n = goal - wide
        store(FACTOR - 1 + goal, jnp.where(n < 0, 0, jnp.where(n == 0, z, 7 + n)))
    for r in range(rows):
        prefix[r] = fields[member, r]
    end = member == FACTOR - 1
    for r in range(rows_slab):
        at = slab * rows_slab + r
        added[r] = jnp.where(end, fields[total, at], residuals[member, at])


def share_kernel(parts, entry, handed, send):
    wide, place2, _ = place()
    last = place2 == FACTOR - 1
    inner = jnp.where(place2 > 0, 1.0, 0.0)
    for j in range(parts.shape[1]):
        outer = jnp.where(last, entry[jnp.maximum(wide - 1, 0), j], handed[j])
        level2 = parts[jnp.maximum(place2 - 1, 0), j] * inner
        for a in range(send.shape[0]):
            for s in range(send.shape[1]):
                send[a, s, 0, j] = outer
                send[a, s, 1, j] = level2


def final_kernel(received, prefix, added, held, coef, ab, out, v):
    wide, place2, member = place()
    slab = lax.axis_index("space")
    rows = coef.shape[1]
    rows_slab = out.shape[1]
    own = received.shape[3]

    def item(which, r):
        return received[r % rows_slab // own, r // rows_slab, which, r % own]

    for r in range(rows):
        v[0, r] = item(0, r)
        v[1, r] = item(0, r)
        v[3, r] = item(1, r)

    def apply(dst, src, level):
        phi(lambda r: v[src, r], lambda r, value: v.__setitem__((dst, r), value), coef, ab, level)

    def body(level):
        def run(n, carry):
            apply(1, 1, level)
            return carry

        return run

    lax.fori_loop(0, place2, body(2), 0)
    for r in range(rows):
        entry = v[1, r] + v[3, r]
        v[1, r] = entry
        v[4, r] = entry
    lax.fori_loop(0, member, body(1), 0)
    for r in range(rows):
        v[1, r] = v[1, r] + prefix[r]
        v[5, r] = jnp.zeros(v.shape[2:], jnp.float32)
    end = member == FACTOR - 1
    both = end & (place2 == FACTOR - 1)
    apply(2, jnp.where(both, 0, jnp.where(end, 4, 1)), jnp.where(both, 3, jnp.where(end, 2, 1)))

    def second(n, carry):
        apply(5, 3, 2)
        return carry

    lax.fori_loop(0, jnp.where(both, 1, 0), second, 0)
    for r in range(rows_slab):
        at = slab * rows_slab + r
        out[3, r] = held[3, r] + (v[2, at] + v[5, at] + added[r])

    def last(i, carry):
        apply(1, 1, 0)
        for r in range(rows_slab):
            out[i, r] = held[i, r] + v[1, slab * rows_slab + r]
        return carry

    lax.fori_loop(0, 3, last, 0)


def call(kernel, inputs, outputs, scratch=(), smem=(), mib=4):
    return pl.pallas_call(
        kernel,
        out_shape=outputs,
        in_specs=[SMEM if i in smem else VMEM for i in range(len(inputs))],
        out_specs=jax.tree.map(lambda _: VMEM, outputs),
        scratch_shapes=[pltpu.VMEM(s, jnp.float32) for s in scratch],
        compiler_params=pltpu.CompilerParams(vmem_limit_bytes=mib << 20),
    )(*inputs)


def local(forcing, start_field, velocity, diffusivity):
    count = lax.axis_size("tm")
    slabs = lax.axis_size("space")
    blocks = count // FACTOR
    wides = blocks // FACTOR
    rows_slab = forcing.shape[1]
    rows = rows_slab * slabs
    own_rows = rows_slab // FACTOR
    tile = forcing.shape[2:]

    near = [[FACTOR * m + j for j in range(FACTOR)] for m in range(blocks)]
    square = [[q * slabs + s for q in group for s in range(slabs)] for group in near]

    def hop(value, pairs):
        moves = []
        for source, target in pairs:
            moves += zip(near[source[0] * FACTOR + source[1]], near[target[0] * FACTOR + target[1]])
        return lax.ppermute(value, "tm", moves)

    own = pl.pallas_call(
        lay_out_kernel,
        out_shape=field(slabs, 8, rows_slab),
        in_specs=[pl.BlockSpec(memory_space=pltpu.HBM)] * 3,
        out_specs=pl.BlockSpec(memory_space=pltpu.HBM),
        scratch_shapes=[pltpu.SemaphoreType.DMA((slabs, 3))],
        compiler_params=pltpu.CompilerParams(vmem_limit_bytes=60 << 20),
    )(forcing, velocity, start_field)
    gathered = lax.all_to_all(own, "space", 0, 0, tiled=True)
    gathered = gathered.reshape((slabs, 8 * rows_slab) + tile)
    last, kept, coef, ab = call(
        chain_kernel,
        (diffusivity, gathered),
        (field(rows), field(4, rows_slab), field(6, rows), field(LEVELS, 2)),
        scratch=[(5, rows) + tile],
        smem=(0,),
        mib=6,
    )
    before = lax.ppermute(last, "tm", [(q, q + 1) for q in range(count - 1)])
    send, held = call(
        residual_kernel,
        (before, kept, coef, ab),
        (field(FACTOR, rows), field(4, rows_slab)),
        scratch=[(5, rows) + tile],
    )
    residuals = lax.all_to_all(send, "tm", 0, 0, axis_index_groups=near, tiled=True)
    parts, prefix, added = call(
        spread_kernel,
        (residuals, coef, ab),
        (field(2 * FACTOR - 1, own_rows), field(rows), field(rows_slab)),
        scratch=[(11, rows) + tile],
        mib=6,
    )
    ends = FACTOR - 1
    third = hop(parts, [((w, 2), (w, 3)) for w in range(wides)])
    pair = parts + hop(parts, [((w, 0), (w, 1)) for w in range(wides)])
    to_last = hop(pair, [((w, 1), (w, 3)) for w in range(wides)])
    to_next = hop(pair, [((w, 1), (w, 2)) for w in range(wides)])
    parts = pair + third + to_last + to_next
    goals = parts[FACTOR - 1 :]
    entry = jnp.zeros_like(goals)
    for w in range(wides - 1):
        entry = entry + hop(goals + entry, [((w, ends), (w + 1, ends))])
    wide = lax.div(lax.axis_index("tm"), count // wides)
    leave = lax.dynamic_slice(goals + entry, (wide, 0, 0, 0), (1,) + goals.shape[1:])[0]
    handed = jnp.zeros_like(leave)
    for i in range(ends):
        handed = handed + hop(leave, [((w, ends), (w + 1, i)) for w in range(wides - 1)])
    send = call(share_kernel, (parts, entry, handed), field(FACTOR, slabs, 2, own_rows))
    send = send.reshape((FACTOR * slabs, 2, own_rows) + tile)
    received = lax.all_to_all(send, ("tm", "space"), 0, 0, axis_index_groups=square, tiled=True)
    received = received.reshape((FACTOR, slabs, 2, own_rows) + tile)
    return call(
        final_kernel,
        (received, prefix, added, held, coef, ab),
        field(4, rows_slab),
        scratch=[(6, rows) + tile],
    )


def solution(mesh):
    if mesh.shape["tm"] != FACTOR**3:
        raise ValueError("time axis")
    placed = (
        P(("grp", "tm"), "space", None, None),
        P(("grp", "space"), None, None),
        P(None, "space", None, None),
        P("grp"),
    )
    return jax.shard_map(
        local,
        mesh=mesh,
        in_specs=placed,
        out_specs=P(("grp", "tm"), "space", None, None),
        check_vma=False,
    )
```

```python
import jax
import jax.numpy as jnp
from jax import lax
from jax.experimental import pallas as pl
from jax.experimental.pallas import tpu as pltpu
from jax.sharding import PartitionSpec as P

SWEEPS = 4
FACTOR = 4
TIME_UNIT = 0.5
LEVELS = 4
VMEM = pl.BlockSpec(memory_space=pltpu.VMEM)
SMEM = pl.BlockSpec(memory_space=pltpu.SMEM)


def field(*lead):
    return jax.ShapeDtypeStruct(lead + (8, 128), jnp.float32)


def phi(get, put, coef, ab, level):
    rows = coef.shape[1]
    a, b = ab[level, 0], ab[level, 1]
    v = [get(r) for r in range(rows)]
    base = None
    for sweep in range(SWEEPS):
        new = []
        for r in range(rows):
            x = v[r]
            t = coef[2, r] * pltpu.roll(x, x.shape[0] - 1, 0) + coef[3, r] * pltpu.roll(x, 1, 0)
            t = t + (coef[4, r] * pltpu.roll(x, x.shape[1] - 1, 1) + coef[5, r] * pltpu.roll(x, 1, 1))
            if r + 1 < rows:
                t = t + coef[0, r] * v[r + 1]
            if r > 0:
                t = t + coef[1, r] * v[r - 1]
            new.append(a * get(r) + b * t)
        v = new
    for r in range(rows):
        put(r, v[r])


def fill_coefficients(coef, ab, velocity_row, kappa):
    rows = coef.shape[1]
    k = jnp.full(coef.shape[2:], kappa, jnp.float32)
    for r in range(rows):
        for axis in range(3):
            half = 0.5 * velocity_row(axis, r)
            coef[2 * axis, r] = k - half
            coef[2 * axis + 1, r] = k + half
    for level in range(LEVELS):
        h = TIME_UNIT * float(FACTOR) ** level
        a = 1.0 / (1.0 + (6.0 * h) * k)
        ab[level, 0] = a
        ab[level, 1] = h * a


def place():
    rank = lax.axis_index("tm")
    block = rank // FACTOR
    return block // FACTOR, block % FACTOR, rank % FACTOR


def chain_kernel(kappa, gathered, last, kept, coef, ab, fields):
    slab = lax.axis_index("space")
    slabs, chunk = gathered.shape[:2]
    rows_slab = chunk // 8
    rows = slabs * rows_slab
    points = 4

    def row(item, r):
        return gathered[r // rows_slab, item * rows_slab + r % rows_slab]

    fill_coefficients(coef, ab, lambda axis, r: row(points + axis, r), kappa[0])
    first = (lax.axis_index("tm") == 0).astype(jnp.float32)
    for r in range(rows):
        fields[0, r] = row(points + 3, r) * first

    def body(n, carry):
        phi(
            lambda r: fields[n, r],
            lambda r, value: fields.__setitem__((n + 1, r), value + row(n, r)),
            coef, ab, 0,
        )
        return carry

    lax.fori_loop(0, points, body, 0)
    for r in range(rows):
        last[r] = fields[points, r]
    for i in range(points):
        for r in range(rows_slab):
            kept[i, r] = fields[1 + i, slab * rows_slab + r]


def residual_kernel(before, kept, coef, ab, send, held, fields):
    slab = lax.axis_index("space")
    rows = coef.shape[1]
    rows_slab = kept.shape[1]
    for r in range(rows):
        fields[0, r] = before[r]

    def body(n, carry):
        phi(
            lambda r: fields[n, r],
            lambda r, value: fields.__setitem__((n + 1, r), value),
            coef, ab, 0,
        )
        return carry

    lax.fori_loop(0, 4, body, 0)
    for r in range(rows):
        value = fields[4, r]
        for j in range(send.shape[0]):
            send[j, r] = value
    for r in range(rows_slab):
        for i in range(3):
            held[i, r] = kept[i, r] + fields[1 + i, slab * rows_slab + r]
        held[3, r] = kept[3, r]


def spread_kernel(residuals, coef, ab, parts, prefix, added, fields):
    wide, place2, member = place()
    slab = lax.axis_index("space")
    rows = coef.shape[1]
    rows_slab = added.shape[0]
    own = parts.shape[1]
    for r in range(rows):
        fields[0, r] = jnp.zeros(fields.shape[2:], jnp.float32)
        fields[1, r] = residuals[0, r]

    def step(src, dst, level, add):
        phi(
            lambda r: fields[src, r],
            lambda r, value: fields.__setitem__((dst, r), add(r, value)),
            coef, ab, level,
        )

    def sums(n, carry):
        step(n, n + 1, 1, lambda r, value: value + residuals[n, r])
        return carry

    lax.fori_loop(1, FACTOR, sums, 0)
    total = FACTOR
    z = total + FACTOR - 1 - place2

    def powers(n, carry):
        src = jnp.where(n == 7, z, n)
        step(src, n + 1, jnp.where(n < 7, 2, 3), lambda r, value: value)
        return carry

    lax.fori_loop(4, 10, powers, 0)

    def store(slot, source):
        for j in range(own):
            parts[slot, j] = fields[source, slab * rows_slab + member * own + j]

    for later in range(1, FACTOR):
        n = later - 1 - place2
        store(later - 1, jnp.where(n >= 0, total + n, 0))
    for goal in range(FACTOR):
        n = goal - wide
        store(FACTOR - 1 + goal, jnp.where(n < 0, 0, jnp.where(n == 0, z, 7 + n)))
    for r in range(rows):
        prefix[r] = fields[member, r]
    end = member == FACTOR - 1
    for r in range(rows_slab):
        at = slab * rows_slab + r
        added[r] = jnp.where(end, fields[total, at], residuals[member, at])


def share_kernel(parts, entry, handed, send):
    wide, place2, _ = place()
    last = place2 == FACTOR - 1
    inner = jnp.where(place2 > 0, 1.0, 0.0)
    for j in range(parts.shape[1]):
        outer = jnp.where(last, entry[jnp.maximum(wide - 1, 0), j], handed[j])
        level2 = parts[jnp.maximum(place2 - 1, 0), j] * inner
        for a in range(send.shape[0]):
            for s in range(send.shape[1]):
                send[a, s, 0, j] = outer
                send[a, s, 1, j] = level2


def final_kernel(received, prefix, added, held, coef, ab, out, v):
    wide, place2, member = place()
    slab = lax.axis_index("space")
    rows = coef.shape[1]
    rows_slab = out.shape[1]
    own = received.shape[3]

    def item(which, r):
        return received[r % rows_slab // own, r // rows_slab, which, r % own]

    for r in range(rows):
        v[0, r] = item(0, r)
        v[1, r] = item(0, r)
        v[3, r] = item(1, r)

    def apply(dst, src, level):
        phi(lambda r: v[src, r], lambda r, value: v.__setitem__((dst, r), value), coef, ab, level)

    def body(level):
        def run(n, carry):
            apply(1, 1, level)
            return carry

        return run

    lax.fori_loop(0, place2, body(2), 0)
    for r in range(rows):
        entry = v[1, r] + v[3, r]
        v[1, r] = entry
        v[4, r] = entry
    lax.fori_loop(0, member, body(1), 0)
    for r in range(rows):
        v[1, r] = v[1, r] + prefix[r]
        v[5, r] = jnp.zeros(v.shape[2:], jnp.float32)
    end = member == FACTOR - 1
    both = end & (place2 == FACTOR - 1)
    apply(2, jnp.where(both, 0, jnp.where(end, 4, 1)), jnp.where(both, 3, jnp.where(end, 2, 1)))

    def second(n, carry):
        apply(5, 3, 2)
        return carry

    lax.fori_loop(0, jnp.where(both, 1, 0), second, 0)
    for r in range(rows_slab):
        at = slab * rows_slab + r
        out[3, r] = held[3, r] + (v[2, at] + v[5, at] + added[r])

    def last(i, carry):
        apply(1, 1, 0)
        for r in range(rows_slab):
            out[i, r] = held[i, r] + v[1, slab * rows_slab + r]
        return carry

    lax.fori_loop(0, 3, last, 0)


def call(kernel, inputs, outputs, scratch=(), smem=(), mib=4):
    return pl.pallas_call(
        kernel,
        out_shape=outputs,
        in_specs=[SMEM if i in smem else VMEM for i in range(len(inputs))],
        out_specs=jax.tree.map(lambda _: VMEM, outputs),
        scratch_shapes=[pltpu.VMEM(s, jnp.float32) for s in scratch],
        compiler_params=pltpu.CompilerParams(vmem_limit_bytes=mib << 20),
    )(*inputs)


def local(forcing, start_field, velocity, diffusivity):
    count = lax.axis_size("tm")
    slabs = lax.axis_size("space")
    blocks = count // FACTOR
    wides = blocks // FACTOR
    rows_slab = forcing.shape[1]
    rows = rows_slab * slabs
    own_rows = rows_slab // FACTOR
    tile = forcing.shape[2:]

    near = [[FACTOR * m + j for j in range(FACTOR)] for m in range(blocks)]
    square = [[q * slabs + s for q in group for s in range(slabs)] for group in near]

    def hop(value, pairs):
        moves = []
        for source, target in pairs:
            moves += zip(near[source[0] * FACTOR + source[1]], near[target[0] * FACTOR + target[1]])
        return lax.ppermute(value, "tm", moves)

    own = jnp.concatenate([forcing, velocity, start_field[None]], axis=0)
    own = own.reshape((1, 8 * rows_slab) + tile)
    gathered = lax.all_to_all(
        jnp.broadcast_to(own, (slabs,) + own.shape[1:]), "space", 0, 0, tiled=True
    )
    last, kept, coef, ab = call(
        chain_kernel,
        (diffusivity, gathered),
        (field(rows), field(4, rows_slab), field(6, rows), field(LEVELS, 2)),
        scratch=[(5, rows) + tile],
        smem=(0,),
        mib=6,
    )
    before = lax.ppermute(last, "tm", [(q, q + 1) for q in range(count - 1)])
    send, held = call(
        residual_kernel,
        (before, kept, coef, ab),
        (field(FACTOR, rows), field(4, rows_slab)),
        scratch=[(5, rows) + tile],
    )
    residuals = lax.all_to_all(send, "tm", 0, 0, axis_index_groups=near, tiled=True)
    parts, prefix, added = call(
        spread_kernel,
        (residuals, coef, ab),
        (field(2 * FACTOR - 1, own_rows), field(rows), field(rows_slab)),
        scratch=[(11, rows) + tile],
        mib=6,
    )
    ends = FACTOR - 1
    third = hop(parts, [((w, 2), (w, 3)) for w in range(wides)])
    pair = parts + hop(parts, [((w, 0), (w, 1)) for w in range(wides)])
    to_last = hop(pair, [((w, 1), (w, 3)) for w in range(wides)])
    to_next = hop(pair, [((w, 1), (w, 2)) for w in range(wides)])
    parts = pair + third + to_last + to_next
    goals = parts[FACTOR - 1 :]
    first = hop(goals, [((0, ends), (1, 0))])
    entry = hop(first, [((1, 0), (1, ends))])
    for w in range(1, wides - 1):
        entry = entry + hop(goals + entry, [((w, ends), (w + 1, ends))])
    wide = lax.div(lax.axis_index("tm"), count // wides)
    leave = lax.dynamic_slice(goals + entry, (wide, 0, 0, 0), (1,) + goals.shape[1:])[0]
    in_first = (wide == 1) & (lax.rem(lax.div(lax.axis_index("tm"), FACTOR), FACTOR) == 0)
    leave = jnp.where(in_first, first[0], leave)
    handed = jnp.where(in_first, first[0], 0.0)
    for i in range(ends):
        pairs = [((w, ends), (w + 1, i)) for w in range(1, wides - 1)]
        handed = handed + hop(leave, pairs + ([((1, 0), (1, i))] if i else []))
    send = call(share_kernel, (parts, entry, handed), field(FACTOR, slabs, 2, own_rows))
    send = send.reshape((FACTOR * slabs, 2, own_rows) + tile)
    received = lax.all_to_all(send, ("tm", "space"), 0, 0, axis_index_groups=square, tiled=True)
    received = received.reshape((FACTOR, slabs, 2, own_rows) + tile)
    return call(
        final_kernel,
        (received, prefix, added, held, coef, ab),
        field(4, rows_slab),
        scratch=[(6, rows) + tile],
    )


def solution(mesh):
    if mesh.shape["tm"] != FACTOR**3:
        raise ValueError("time axis")
    placed = (
        P(("grp", "tm"), "space", None, None),
        P(("grp", "space"), None, None),
        P(None, "space", None, None),
        P("grp"),
    )
    return jax.shard_map(
        local,
        mesh=mesh,
        in_specs=placed,
        out_specs=P(("grp", "tm"), "space", None, None),
        check_vma=False,
    )
```

```python
import jax
import jax.numpy as jnp
from jax import lax
from jax.experimental import pallas as pl
from jax.experimental.pallas import tpu as pltpu
from jax.sharding import PartitionSpec as P

SWEEPS = 4
FACTOR = 4
TIME_UNIT = 0.5
LEVELS = 4
VMEM = pl.BlockSpec(memory_space=pltpu.VMEM)
SMEM = pl.BlockSpec(memory_space=pltpu.SMEM)


def field(*lead):
    return jax.ShapeDtypeStruct(lead + (8, 128), jnp.float32)


def phi(get, put, coef, ab, level):
    rows = coef.shape[1]
    a, b = ab[level, 0], ab[level, 1]
    v = [get(r) for r in range(rows)]
    base = None
    for sweep in range(SWEEPS):
        new = []
        for r in range(rows):
            x = v[r]
            t = coef[2, r] * pltpu.roll(x, x.shape[0] - 1, 0) + coef[3, r] * pltpu.roll(x, 1, 0)
            t = t + (coef[4, r] * pltpu.roll(x, x.shape[1] - 1, 1) + coef[5, r] * pltpu.roll(x, 1, 1))
            if r + 1 < rows:
                t = t + coef[0, r] * v[r + 1]
            if r > 0:
                t = t + coef[1, r] * v[r - 1]
            new.append(a * get(r) + b * t)
        v = new
    for r in range(rows):
        put(r, v[r])


def fill_coefficients(coef, ab, velocity_row, kappa):
    rows = coef.shape[1]
    k = jnp.full(coef.shape[2:], kappa, jnp.float32)
    for r in range(rows):
        for axis in range(3):
            half = 0.5 * velocity_row(axis, r)
            coef[2 * axis, r] = k - half
            coef[2 * axis + 1, r] = k + half
    for level in range(LEVELS):
        h = TIME_UNIT * float(FACTOR) ** level
        a = 1.0 / (1.0 + (6.0 * h) * k)
        ab[level, 0] = a
        ab[level, 1] = h * a


def place():
    rank = lax.axis_index("tm")
    block = rank // FACTOR
    return block // FACTOR, block % FACTOR, rank % FACTOR


def chain_kernel(kappa, gathered, last, kept, coef, ab, fields):
    slab = lax.axis_index("space")
    slabs, chunk = gathered.shape[:2]
    rows_slab = chunk // 8
    rows = slabs * rows_slab
    points = 4

    def row(item, r):
        return gathered[r // rows_slab, item * rows_slab + r % rows_slab]

    fill_coefficients(coef, ab, lambda axis, r: row(points + axis, r), kappa[0])
    first = (lax.axis_index("tm") == 0).astype(jnp.float32)
    for r in range(rows):
        fields[0, r] = row(points + 3, r) * first

    def body(n, carry):
        phi(
            lambda r: fields[n, r],
            lambda r, value: fields.__setitem__((n + 1, r), value + row(n, r)),
            coef, ab, 0,
        )
        return carry

    lax.fori_loop(0, points, body, 0)
    for r in range(rows):
        last[r] = fields[points, r]
    for i in range(points):
        for r in range(rows_slab):
            kept[i, r] = fields[1 + i, slab * rows_slab + r]


def residual_kernel(before, kept, coef, ab, residual, held, fields):
    slab = lax.axis_index("space")
    rows = coef.shape[1]
    rows_slab = kept.shape[1]
    for r in range(rows):
        fields[0, r] = before[r]

    def body(n, carry):
        phi(
            lambda r: fields[n, r],
            lambda r, value: fields.__setitem__((n + 1, r), value),
            coef, ab, 0,
        )
        return carry

    lax.fori_loop(0, 4, body, 0)
    for r in range(rows):
        residual[r] = fields[4, r]
    for r in range(rows_slab):
        for i in range(3):
            held[i, r] = kept[i, r] + fields[1 + i, slab * rows_slab + r]
        held[3, r] = kept[3, r]


def spread_kernel(residuals, coef, ab, parts, prefix, added, fields):
    wide, place2, member = place()
    slab = lax.axis_index("space")
    rows = coef.shape[1]
    rows_slab = added.shape[0]
    own = parts.shape[1]
    for r in range(rows):
        fields[0, r] = jnp.zeros(fields.shape[2:], jnp.float32)
        fields[1, r] = residuals[0, r]

    def step(src, dst, level, add):
        phi(
            lambda r: fields[src, r],
            lambda r, value: fields.__setitem__((dst, r), add(r, value)),
            coef, ab, level,
        )

    def sums(n, carry):
        step(n, n + 1, 1, lambda r, value: value + residuals[n, r])
        return carry

    lax.fori_loop(1, FACTOR, sums, 0)
    total = FACTOR
    z = total + FACTOR - 1 - place2

    def powers(n, carry):
        src = jnp.where(n == 7, z, n)
        step(src, n + 1, jnp.where(n < 7, 2, 3), lambda r, value: value)
        return carry

    lax.fori_loop(4, 10, powers, 0)

    def store(slot, source):
        for j in range(own):
            parts[slot, j] = fields[source, slab * rows_slab + member * own + j]

    for later in range(1, FACTOR):
        n = later - 1 - place2
        store(later - 1, jnp.where(n >= 0, total + n, 0))
    for goal in range(FACTOR):
        n = goal - wide
        store(FACTOR - 1 + goal, jnp.where(n < 0, 0, jnp.where(n == 0, z, 7 + n)))
    for r in range(rows):
        prefix[r] = fields[member, r]
    end = member == FACTOR - 1
    for r in range(rows_slab):
        at = slab * rows_slab + r
        added[r] = jnp.where(end, fields[total, at], residuals[member, at])


def share_kernel(parts, entry, send):
    _, place2, _ = place()
    inner = jnp.where(place2 > 0, 1.0, 0.0)
    for j in range(parts.shape[1]):
        outer = entry[j]
        level2 = parts[jnp.maximum(place2 - 1, 0), j] * inner
        for a in range(send.shape[0]):
            for s in range(send.shape[1]):
                send[a, s, 0, j] = outer
                send[a, s, 1, j] = level2


def final_kernel(received, prefix, added, held, coef, ab, out, v):
    wide, place2, member = place()
    slab = lax.axis_index("space")
    rows = coef.shape[1]
    rows_slab = out.shape[1]
    own = received.shape[3]

    def item(which, r):
        return received[r % rows_slab // own, r // rows_slab, which, r % own]

    for r in range(rows):
        v[0, r] = item(0, r)
        v[1, r] = item(0, r)
        v[3, r] = item(1, r)

    def apply(dst, src, level):
        phi(lambda r: v[src, r], lambda r, value: v.__setitem__((dst, r), value), coef, ab, level)

    def body(level):
        def run(n, carry):
            apply(1, 1, level)
            return carry

        return run

    lax.fori_loop(0, place2, body(2), 0)
    for r in range(rows):
        entry = v[1, r] + v[3, r]
        v[1, r] = entry
        v[4, r] = entry
    lax.fori_loop(0, member, body(1), 0)
    for r in range(rows):
        v[1, r] = v[1, r] + prefix[r]
        v[5, r] = jnp.zeros(v.shape[2:], jnp.float32)
    end = member == FACTOR - 1
    both = end & (place2 == FACTOR - 1)
    apply(2, jnp.where(both, 0, jnp.where(end, 4, 1)), jnp.where(both, 3, jnp.where(end, 2, 1)))

    def second(n, carry):
        apply(5, 3, 2)
        return carry

    lax.fori_loop(0, jnp.where(both, 1, 0), second, 0)
    for r in range(rows_slab):
        at = slab * rows_slab + r
        out[3, r] = held[3, r] + (v[2, at] + v[5, at] + added[r])

    def last(i, carry):
        apply(1, 1, 0)
        for r in range(rows_slab):
            out[i, r] = held[i, r] + v[1, slab * rows_slab + r]
        return carry

    lax.fori_loop(0, 3, last, 0)


def call(kernel, inputs, outputs, scratch=(), smem=(), mib=4):
    return pl.pallas_call(
        kernel,
        out_shape=outputs,
        in_specs=[SMEM if i in smem else VMEM for i in range(len(inputs))],
        out_specs=jax.tree.map(lambda _: VMEM, outputs),
        scratch_shapes=[pltpu.VMEM(s, jnp.float32) for s in scratch],
        compiler_params=pltpu.CompilerParams(vmem_limit_bytes=mib << 20),
    )(*inputs)


def local(forcing, start_field, velocity, diffusivity):
    count = lax.axis_size("tm")
    slabs = lax.axis_size("space")
    blocks = count // FACTOR
    wides = blocks // FACTOR
    rows_slab = forcing.shape[1]
    rows = rows_slab * slabs
    own_rows = rows_slab // FACTOR
    tile = forcing.shape[2:]

    near = [[FACTOR * m + j for j in range(FACTOR)] for m in range(blocks)]
    square = [[q * slabs + s for q in group for s in range(slabs)] for group in near]

    def hop(value, pairs):
        moves = []
        for source, target in pairs:
            moves += zip(near[source[0] * FACTOR + source[1]], near[target[0] * FACTOR + target[1]])
        return lax.ppermute(value, "tm", moves)

    own = jnp.concatenate([forcing, velocity, start_field[None]], axis=0)
    own = own.reshape((1, 8 * rows_slab) + tile)
    gathered = lax.all_to_all(
        jnp.broadcast_to(own, (slabs,) + own.shape[1:]), "space", 0, 0, tiled=True
    )
    last, kept, coef, ab = call(
        chain_kernel,
        (diffusivity, gathered),
        (field(rows), field(4, rows_slab), field(6, rows), field(LEVELS, 2)),
        scratch=[(5, rows) + tile],
        smem=(0,),
        mib=6,
    )
    before = lax.ppermute(last, "tm", [(q, q + 1) for q in range(count - 1)])
    residual, held = call(
        residual_kernel,
        (before, kept, coef, ab),
        (field(rows), field(4, rows_slab)),
        scratch=[(5, rows) + tile],
    )
    residuals = lax.all_gather(residual, "tm", axis_index_groups=near)
    parts, prefix, added = call(
        spread_kernel,
        (residuals, coef, ab),
        (field(2 * FACTOR - 1, own_rows), field(rows), field(rows_slab)),
        scratch=[(11, rows) + tile],
        mib=6,
    )
    ends = FACTOR - 1
    third = hop(parts, [((w, 2), (w, 3)) for w in range(wides)])
    pair = parts + hop(parts, [((w, 0), (w, 1)) for w in range(wides)])
    to_last = hop(pair, [((w, 1), (w, 3)) for w in range(wides)])
    to_next = hop(pair, [((w, 1), (w, 2)) for w in range(wides)])
    parts = pair + third + to_last + to_next
    goals = parts[FACTOR - 1 :]
    first = hop(goals, [((0, ends), (1, 0))])
    rank = lax.axis_index("tm")
    wide = lax.div(rank, count // wides)

    def carry_on(goals, first):
        entry = hop(first, [((1, 0), (1, ends))])
        for w in range(1, wides - 1):
            entry = entry + hop(goals + entry, [((w, ends), (w + 1, ends))])
        leave = lax.dynamic_slice(goals + entry, (wide, 0, 0, 0), (1,) + goals.shape[1:])[0]
        in_first = (wide == 1) & (lax.rem(lax.div(rank, FACTOR), FACTOR) == 0)
        leave = jnp.where(in_first, first[0], leave)
        handed = jnp.where(in_first, first[0], 0.0)
        for i in range(ends):
            pairs = [((w, ends), (w + 1, i)) for w in range(1, wides - 1)]
            handed = handed + hop(leave, pairs + ([((1, 0), (1, i))] if i else []))
        last = lax.dynamic_slice(entry, (wide - 1, 0, 0, 0), (1,) + goals.shape[1:])[0]
        return jnp.where(lax.rem(lax.div(rank, FACTOR), FACTOR) == ends, last, handed)

    entry = lax.cond(wide > 0, carry_on, lambda goals, first: jnp.zeros_like(goals[0]), goals, first)
    send = call(share_kernel, (parts, entry), field(FACTOR, slabs, 2, own_rows))
    send = send.reshape((FACTOR * slabs, 2, own_rows) + tile)
    received = lax.all_to_all(send, ("tm", "space"), 0, 0, axis_index_groups=square, tiled=True)
    received = received.reshape((FACTOR, slabs, 2, own_rows) + tile)
    return call(
        final_kernel,
        (received, prefix, added, held, coef, ab),
        field(4, rows_slab),
        scratch=[(6, rows) + tile],
    )


def solution(mesh):
    if mesh.shape["tm"] != FACTOR**3:
        raise ValueError("time axis")
    placed = (
        P(("grp", "tm"), "space", None, None),
        P(("grp", "space"), None, None),
        P(None, "space", None, None),
        P("grp"),
    )
    return jax.shard_map(
        local,
        mesh=mesh,
        in_specs=placed,
        out_specs=P(("grp", "tm"), "space", None, None),
        check_vma=False,
    )
```

```python
import jax
import jax.numpy as jnp
from jax import lax
from jax.experimental import pallas as pl
from jax.experimental.pallas import tpu as pltpu
from jax.sharding import PartitionSpec as P

SWEEPS = 4
FACTOR = 4
TIME_UNIT = 0.5
LEVELS = 4
VMEM = pl.BlockSpec(memory_space=pltpu.VMEM)
SMEM = pl.BlockSpec(memory_space=pltpu.SMEM)


def field(*lead):
    return jax.ShapeDtypeStruct(lead + (8, 128), jnp.float32)


def phi(get, put, coef, ab, level):
    rows = coef.shape[1]
    a, b = ab[level, 0], ab[level, 1]
    v = [get(r) for r in range(rows)]
    base = None
    for sweep in range(SWEEPS):
        new = []
        for r in range(rows):
            x = v[r]
            t = coef[2, r] * pltpu.roll(x, x.shape[0] - 1, 0) + coef[3, r] * pltpu.roll(x, 1, 0)
            t = t + (coef[4, r] * pltpu.roll(x, x.shape[1] - 1, 1) + coef[5, r] * pltpu.roll(x, 1, 1))
            if r + 1 < rows:
                t = t + coef[0, r] * v[r + 1]
            if r > 0:
                t = t + coef[1, r] * v[r - 1]
            new.append(a * get(r) + b * t)
        v = new
    for r in range(rows):
        put(r, v[r])


def fill_coefficients(coef, ab, velocity_row, kappa):
    rows = coef.shape[1]
    k = jnp.full(coef.shape[2:], kappa, jnp.float32)
    for r in range(rows):
        for axis in range(3):
            half = 0.5 * velocity_row(axis, r)
            coef[2 * axis, r] = k - half
            coef[2 * axis + 1, r] = k + half
    for level in range(LEVELS):
        h = TIME_UNIT * float(FACTOR) ** level
        a = 1.0 / (1.0 + (6.0 * h) * k)
        ab[level, 0] = a
        ab[level, 1] = h * a


def place():
    rank = lax.axis_index("tm")
    block = rank // FACTOR
    return block // FACTOR, block % FACTOR, rank % FACTOR


def chain_kernel(kappa, gathered, last, kept, coef, ab, fields):
    slab = lax.axis_index("space")
    slabs, chunk = gathered.shape[:2]
    rows_slab = chunk // 8
    rows = slabs * rows_slab
    points = 4

    def row(item, r):
        return gathered[r // rows_slab, item * rows_slab + r % rows_slab]

    fill_coefficients(coef, ab, lambda axis, r: row(points + axis, r), kappa[0])
    first = (lax.axis_index("tm") == 0).astype(jnp.float32)
    for r in range(rows):
        fields[0, r] = row(points + 3, r) * first

    def body(n, carry):
        phi(
            lambda r: fields[n, r],
            lambda r, value: fields.__setitem__((n + 1, r), value + row(n, r)),
            coef, ab, 0,
        )
        return carry

    lax.fori_loop(0, points, body, 0)
    for r in range(rows):
        last[r] = fields[points, r]
    for i in range(points):
        for r in range(rows_slab):
            kept[i, r] = fields[1 + i, slab * rows_slab + r]


def residual_kernel(before, kept, coef, ab, residual, held, fields):
    slab = lax.axis_index("space")
    rows = coef.shape[1]
    rows_slab = kept.shape[1]
    for r in range(rows):
        fields[0, r] = before[r]

    def body(n, carry):
        phi(
            lambda r: fields[n, r],
            lambda r, value: fields.__setitem__((n + 1, r), value),
            coef, ab, 0,
        )
        return carry

    lax.fori_loop(0, 4, body, 0)
    for r in range(rows):
        residual[r] = fields[4, r]
    for r in range(rows_slab):
        for i in range(3):
            held[i, r] = kept[i, r] + fields[1 + i, slab * rows_slab + r]
        held[3, r] = kept[3, r]


def spread_kernel(residuals, coef, ab, parts, prefix, added, fields):
    wide, place2, member = place()
    slab = lax.axis_index("space")
    rows = coef.shape[1]
    rows_slab = added.shape[0]
    own = parts.shape[1]
    for r in range(rows):
        fields[0, r] = jnp.zeros(fields.shape[2:], jnp.float32)
        fields[1, r] = residuals[0, r]

    def step(src, dst, level, add):
        phi(
            lambda r: fields[src, r],
            lambda r, value: fields.__setitem__((dst, r), add(r, value)),
            coef, ab, level,
        )

    def sums(n, carry):
        step(n, n + 1, 1, lambda r, value: value + residuals[n, r])
        return carry

    lax.fori_loop(1, FACTOR, sums, 0)
    total = FACTOR
    z = total + FACTOR - 1 - place2

    def powers(n, carry):
        src = jnp.where(n == 7, z, n)
        step(src, n + 1, jnp.where(n < 7, 2, 3), lambda r, value: value)
        return carry

    lax.fori_loop(4, 10, powers, 0)

    def store(slot, source):
        for j in range(own):
            parts[slot, j] = fields[source, slab * rows_slab + member * own + j]

    for later in range(1, FACTOR):
        n = later - 1 - place2
        store(later - 1, jnp.where(n >= 0, total + n, 0))
    for goal in range(FACTOR):
        n = goal - wide
        store(FACTOR - 1 + goal, jnp.where(n < 0, 0, jnp.where(n == 0, z, 7 + n)))
    for r in range(rows):
        prefix[r] = fields[member, r]
    end = member == FACTOR - 1
    for r in range(rows_slab):
        at = slab * rows_slab + r
        added[r] = jnp.where(end, fields[total, at], residuals[member, at])


def share_kernel(level2, entry, send):
    for j in range(entry.shape[0]):
        for a in range(send.shape[0]):
            for s in range(send.shape[1]):
                send[a, s, 0, j] = entry[j]
                send[a, s, 1, j] = level2[j]


def final_kernel(received, prefix, added, held, coef, ab, out, v):
    wide, place2, member = place()
    slab = lax.axis_index("space")
    rows = coef.shape[1]
    rows_slab = out.shape[1]
    own = received.shape[3]

    def item(which, r):
        return received[r % rows_slab // own, r // rows_slab, which, r % own]

    for r in range(rows):
        v[0, r] = item(0, r)
        v[1, r] = item(0, r)
        v[3, r] = item(1, r)

    def apply(dst, src, level):
        phi(lambda r: v[src, r], lambda r, value: v.__setitem__((dst, r), value), coef, ab, level)

    def body(level):
        def run(n, carry):
            apply(1, 1, level)
            return carry

        return run

    lax.fori_loop(0, place2, body(2), 0)
    for r in range(rows):
        entry = v[1, r] + v[3, r]
        v[1, r] = entry
        v[4, r] = entry
    lax.fori_loop(0, member, body(1), 0)
    for r in range(rows):
        v[1, r] = v[1, r] + prefix[r]
        v[5, r] = jnp.zeros(v.shape[2:], jnp.float32)
    end = member == FACTOR - 1
    both = end & (place2 == FACTOR - 1)
    apply(2, jnp.where(both, 0, jnp.where(end, 4, 1)), jnp.where(both, 3, jnp.where(end, 2, 1)))

    def second(n, carry):
        apply(5, 3, 2)
        return carry

    lax.fori_loop(0, jnp.where(both, 1, 0), second, 0)
    for r in range(rows_slab):
        at = slab * rows_slab + r
        out[3, r] = held[3, r] + (v[2, at] + v[5, at] + added[r])

    def last(i, carry):
        apply(1, 1, 0)
        for r in range(rows_slab):
            out[i, r] = held[i, r] + v[1, slab * rows_slab + r]
        return carry

    lax.fori_loop(0, 3, last, 0)


def call(kernel, inputs, outputs, scratch=(), smem=(), mib=4):
    return pl.pallas_call(
        kernel,
        out_shape=outputs,
        in_specs=[SMEM if i in smem else VMEM for i in range(len(inputs))],
        out_specs=jax.tree.map(lambda _: VMEM, outputs),
        scratch_shapes=[pltpu.VMEM(s, jnp.float32) for s in scratch],
        compiler_params=pltpu.CompilerParams(vmem_limit_bytes=mib << 20),
    )(*inputs)


def local(forcing, start_field, velocity, diffusivity):
    count = lax.axis_size("tm")
    slabs = lax.axis_size("space")
    blocks = count // FACTOR
    wides = blocks // FACTOR
    rows_slab = forcing.shape[1]
    rows = rows_slab * slabs
    own_rows = rows_slab // FACTOR
    tile = forcing.shape[2:]

    near = [[FACTOR * m + j for j in range(FACTOR)] for m in range(blocks)]
    square = [[q * slabs + s for q in group for s in range(slabs)] for group in near]

    def hop(value, pairs):
        moves = []
        for source, target in pairs:
            moves += zip(near[source[0] * FACTOR + source[1]], near[target[0] * FACTOR + target[1]])
        return lax.ppermute(value, "tm", moves)

    own = jnp.concatenate([forcing, velocity, start_field[None]], axis=0)
    own = own.reshape((1, 8 * rows_slab) + tile)
    gathered = lax.all_to_all(
        jnp.broadcast_to(own, (slabs,) + own.shape[1:]), "space", 0, 0, tiled=True
    )
    last, kept, coef, ab = call(
        chain_kernel,
        (diffusivity, gathered),
        (field(rows), field(4, rows_slab), field(6, rows), field(LEVELS, 2)),
        scratch=[(5, rows) + tile],
        smem=(0,),
        mib=6,
    )
    before = lax.ppermute(last, "tm", [(q, q + 1) for q in range(count - 1)])
    residual, held = call(
        residual_kernel,
        (before, kept, coef, ab),
        (field(rows), field(4, rows_slab)),
        scratch=[(5, rows) + tile],
    )
    residuals = lax.all_gather(residual, "tm", axis_index_groups=near)
    parts, prefix, added = call(
        spread_kernel,
        (residuals, coef, ab),
        (field(2 * FACTOR - 1, own_rows), field(rows), field(rows_slab)),
        scratch=[(11, rows) + tile],
        mib=6,
    )
    ends = FACTOR - 1
    rank = lax.axis_index("tm")
    wide = lax.div(rank, count // wides)
    place2 = lax.rem(lax.div(rank, FACTOR), FACTOR)

    def message(parts, start):
        return lax.dynamic_slice(parts, (start, 0, 0, 0), (FACTOR + 1,) + parts.shape[1:])

    def inside(value, pairs, block2s):
        return hop(value, [((w, i), (w, j)) for w in block2s for i, j in pairs])

    def direct(parts):
        block2s = range(1)
        summed = inside(parts[ends - 1 :], [(0, 3)], block2s)
        summed = summed + inside(message(parts, jnp.minimum(place2 + 1, 2)), [(0, 2), (1, 3)], block2s)
        summed = summed + inside(message(parts, jnp.minimum(place2, 2)), [(0, 1), (2, 3)], block2s)
        summed = summed + inside(parts[1 : FACTOR + 2], [(1, 2)], block2s)
        return (summed[0], *(parts[ends + i] + summed[1 + i] for i in range(FACTOR)))

    def tree(parts):
        block2s = range(1, wides)

        def early(parts):
            got = inside(parts, [(0, 1)], block2s)
            return tuple(got[i] for i in range(2 * FACTOR - 1))

        none = jnp.zeros_like(parts[0])
        got = lax.cond(place2 <= 1, early, lambda parts: (none,) * (2 * FACTOR - 1), parts)
        pair = parts + jnp.stack(got)

        def late(pair, parts):
            third = inside(parts[ends - 1 :], [(2, 3)], block2s)
            fourth = inside(pair[ends - 1 :], [(1, 3)], block2s)
            next_ = inside(pair[1], [(1, 2)], block2s)
            both = third + fourth
            return (both[0] + next_, *(both[1 + i] for i in range(FACTOR)))

        first2, *got4 = lax.cond(place2 >= 1, late, lambda pair, parts: (none,) * (FACTOR + 1), pair, parts)
        return (jnp.where(place2 == 1, got[0], first2), *(pair[ends + i] + got4[i] for i in range(FACTOR)))

    level2, *goals = lax.cond(wide > 0, tree, direct, parts)
    goals = jnp.stack(goals)
    first = hop(goals, [((0, ends), (1, 0))])

    def carry_on(goals, first):
        entry = hop(first, [((1, 0), (1, ends))])

        def between(goals, entry):
            for w in range(1, wides - 1):
                entry = entry + hop(goals + entry, [((w, ends), (w + 1, ends))])
            size = (1,) + goals.shape[1:]
            return (
                lax.dynamic_slice(goals + entry, (wide, 0, 0, 0), size)[0],
                lax.dynamic_slice(entry, (wide - 1, 0, 0, 0), size)[0],
            )

        leave, own = lax.cond(
            place2 == ends, between, lambda goals, entry: (first[0], first[0]), goals, entry
        )
        for i in range(ends):
            pairs = [((w, ends), (w + 1, i)) for w in range(1, wides - 1)]
            own = own + hop(leave, pairs + ([((1, 0), (1, i))] if i else []))
        return own

    entry = lax.cond(wide > 0, carry_on, lambda goals, first: jnp.zeros_like(goals[0]), goals, first)
    send = call(share_kernel, (level2, entry), field(FACTOR, slabs, 2, own_rows))
    send = send.reshape((FACTOR * slabs, 2, own_rows) + tile)
    received = lax.all_to_all(send, ("tm", "space"), 0, 0, axis_index_groups=square, tiled=True)
    received = received.reshape((FACTOR, slabs, 2, own_rows) + tile)
    return call(
        final_kernel,
        (received, prefix, added, held, coef, ab),
        field(4, rows_slab),
        scratch=[(6, rows) + tile],
    )


def solution(mesh):
    if mesh.shape["tm"] != FACTOR**3:
        raise ValueError("time axis")
    placed = (
        P(("grp", "tm"), "space", None, None),
        P(("grp", "space"), None, None),
        P(None, "space", None, None),
        P("grp"),
    )
    return jax.shard_map(
        local,
        mesh=mesh,
        in_specs=placed,
        out_specs=P(("grp", "tm"), "space", None, None),
        check_vma=False,
    )
```

```python
import jax
import jax.numpy as jnp
from jax import lax
from jax.experimental import pallas as pl
from jax.experimental.pallas import tpu as pltpu
from jax.sharding import PartitionSpec as P

SWEEPS = 4
FACTOR = 4
TIME_UNIT = 0.5
LEVELS = 4
VMEM = pl.BlockSpec(memory_space=pltpu.VMEM)
SMEM = pl.BlockSpec(memory_space=pltpu.SMEM)


def field(*lead):
    return jax.ShapeDtypeStruct(lead + (8, 128), jnp.float32)


def phi(get, put, coef, ab, level):
    rows = coef.shape[1]
    a, b = ab[level, 0], ab[level, 1]
    v = [get(r) for r in range(rows)]
    base = None
    for sweep in range(SWEEPS):
        new = []
        for r in range(rows):
            x = v[r]
            t = coef[2, r] * pltpu.roll(x, x.shape[0] - 1, 0) + coef[3, r] * pltpu.roll(x, 1, 0)
            t = t + (coef[4, r] * pltpu.roll(x, x.shape[1] - 1, 1) + coef[5, r] * pltpu.roll(x, 1, 1))
            if r + 1 < rows:
                t = t + coef[0, r] * v[r + 1]
            if r > 0:
                t = t + coef[1, r] * v[r - 1]
            new.append(a * get(r) + b * t)
        v = new
    for r in range(rows):
        put(r, v[r])


def fill_coefficients(coef, ab, velocity_row, kappa):
    rows = coef.shape[1]
    k = jnp.full(coef.shape[2:], kappa, jnp.float32)
    for r in range(rows):
        for axis in range(3):
            half = 0.5 * velocity_row(axis, r)
            coef[2 * axis, r] = k - half
            coef[2 * axis + 1, r] = k + half
    for level in range(LEVELS):
        h = TIME_UNIT * float(FACTOR) ** level
        a = 1.0 / (1.0 + (6.0 * h) * k)
        ab[level, 0] = a
        ab[level, 1] = h * a


def place():
    rank = lax.axis_index("tm")
    block = rank // FACTOR
    return block // FACTOR, block % FACTOR, rank % FACTOR


def chain_kernel(kappa, gathered, last, kept, coef, ab, fields):
    slab = lax.axis_index("space")
    slabs, chunk = gathered.shape[:2]
    rows_slab = chunk // 8
    rows = slabs * rows_slab
    points = 4

    def row(item, r):
        return gathered[r // rows_slab, item * rows_slab + r % rows_slab]

    fill_coefficients(coef, ab, lambda axis, r: row(points + axis, r), kappa[0])
    first = (lax.axis_index("tm") == 0).astype(jnp.float32)
    for r in range(rows):
        fields[0, r] = row(points + 3, r) * first

    def body(n, carry):
        phi(
            lambda r: fields[n, r],
            lambda r, value: fields.__setitem__((n + 1, r), value + row(n, r)),
            coef, ab, 0,
        )
        return carry

    lax.fori_loop(0, points, body, 0)
    for r in range(rows):
        last[r] = fields[points, r]
    for i in range(points):
        for r in range(rows_slab):
            kept[i, r] = fields[1 + i, slab * rows_slab + r]


def residual_kernel(before, kept, coef, ab, residual, held, fields):
    slab = lax.axis_index("space")
    rows = coef.shape[1]
    rows_slab = kept.shape[1]
    for r in range(rows):
        fields[0, r] = before[r]

    def body(n, carry):
        phi(
            lambda r: fields[n, r],
            lambda r, value: fields.__setitem__((n + 1, r), value),
            coef, ab, 0,
        )
        return carry

    lax.fori_loop(0, 4, body, 0)
    for r in range(rows):
        residual[r] = fields[4, r]
    for r in range(rows_slab):
        for i in range(3):
            held[i, r] = kept[i, r] + fields[1 + i, slab * rows_slab + r]
        held[3, r] = kept[3, r]


def spread_kernel(residuals, coef, ab, parts, prefix, added, fields):
    wide, place2, member = place()
    slab = lax.axis_index("space")
    rows = coef.shape[1]
    rows_slab = added.shape[0]
    own = parts.shape[1]
    for r in range(rows):
        fields[0, r] = jnp.zeros(fields.shape[2:], jnp.float32)
        fields[1, r] = residuals[0, r]

    def step(src, dst, level, add):
        phi(
            lambda r: fields[src, r],
            lambda r, value: fields.__setitem__((dst, r), add(r, value)),
            coef, ab, level,
        )

    def sums(n, carry):
        step(n, n + 1, 1, lambda r, value: value + residuals[n, r])
        return carry

    lax.fori_loop(1, FACTOR, sums, 0)
    total = FACTOR
    z = total + FACTOR - 1 - place2

    def powers(n, carry):
        src = jnp.where(n == 7, z, n)
        step(src, n + 1, jnp.where(n < 7, 2, 3), lambda r, value: value)
        return carry

    lax.fori_loop(4, 9, powers, 0)

    def store(slot, source):
        for j in range(own):
            parts[slot, j] = fields[source, slab * rows_slab + member * own + j]

    for later in range(1, FACTOR):
        n = later - 1 - place2
        store(later - 1, jnp.where(n >= 0, total + n, 0))
    for goal in range(FACTOR - 1):
        n = goal - wide
        store(FACTOR - 1 + goal, jnp.where(n < 0, 0, jnp.where(n == 0, z, 7 + n)))
    for r in range(rows):
        prefix[r] = fields[member, r]
    end = member == FACTOR - 1
    for r in range(rows_slab):
        at = slab * rows_slab + r
        added[r] = jnp.where(end, fields[total, at], residuals[member, at])


def share_kernel(level2, entry, send):
    for j in range(entry.shape[0]):
        for a in range(send.shape[0]):
            for s in range(send.shape[1]):
                send[a, s, 0, j] = entry[j]
                send[a, s, 1, j] = level2[j]


def final_kernel(received, prefix, added, held, coef, ab, out, v):
    wide, place2, member = place()
    slab = lax.axis_index("space")
    rows = coef.shape[1]
    rows_slab = out.shape[1]
    own = received.shape[3]

    def item(which, r):
        return received[r % rows_slab // own, r // rows_slab, which, r % own]

    for r in range(rows):
        v[0, r] = item(0, r)
        v[1, r] = item(0, r)
        v[3, r] = item(1, r)

    def apply(dst, src, level):
        phi(lambda r: v[src, r], lambda r, value: v.__setitem__((dst, r), value), coef, ab, level)

    def body(level):
        def run(n, carry):
            apply(1, 1, level)
            return carry

        return run

    lax.fori_loop(0, place2, body(2), 0)
    for r in range(rows):
        entry = v[1, r] + v[3, r]
        v[1, r] = entry
        v[4, r] = entry
    lax.fori_loop(0, member, body(1), 0)
    for r in range(rows):
        v[1, r] = v[1, r] + prefix[r]
        v[5, r] = jnp.zeros(v.shape[2:], jnp.float32)
    end = member == FACTOR - 1
    both = end & (place2 == FACTOR - 1)
    apply(2, jnp.where(both, 0, jnp.where(end, 4, 1)), jnp.where(both, 3, jnp.where(end, 2, 1)))

    def second(n, carry):
        apply(5, 3, 2)
        return carry

    lax.fori_loop(0, jnp.where(both, 1, 0), second, 0)
    for r in range(rows_slab):
        at = slab * rows_slab + r
        out[3, r] = held[3, r] + (v[2, at] + v[5, at] + added[r])

    def last(i, carry):
        apply(1, 1, 0)
        for r in range(rows_slab):
            out[i, r] = held[i, r] + v[1, slab * rows_slab + r]
        return carry

    lax.fori_loop(0, 3, last, 0)


def call(kernel, inputs, outputs, scratch=(), smem=(), mib=4):
    return pl.pallas_call(
        kernel,
        out_shape=outputs,
        in_specs=[SMEM if i in smem else VMEM for i in range(len(inputs))],
        out_specs=jax.tree.map(lambda _: VMEM, outputs),
        scratch_shapes=[pltpu.VMEM(s, jnp.float32) for s in scratch],
        compiler_params=pltpu.CompilerParams(vmem_limit_bytes=mib << 20),
    )(*inputs)


def local(forcing, start_field, velocity, diffusivity):
    count = lax.axis_size("tm")
    slabs = lax.axis_size("space")
    blocks = count // FACTOR
    wides = blocks // FACTOR
    rows_slab = forcing.shape[1]
    rows = rows_slab * slabs
    own_rows = rows_slab // FACTOR
    tile = forcing.shape[2:]

    near = [[FACTOR * m + j for j in range(FACTOR)] for m in range(blocks)]
    square = [[q * slabs + s for q in group for s in range(slabs)] for group in near]

    def hop(value, pairs):
        moves = []
        for source, target in pairs:
            moves += zip(near[source[0] * FACTOR + source[1]], near[target[0] * FACTOR + target[1]])
        return lax.ppermute(value, "tm", moves)

    own = jnp.concatenate([forcing, velocity, start_field[None]], axis=0)
    own = own.reshape((1, 8 * rows_slab) + tile)
    gathered = lax.all_to_all(
        jnp.broadcast_to(own, (slabs,) + own.shape[1:]), "space", 0, 0, tiled=True
    )
    last, kept, coef, ab = call(
        chain_kernel,
        (diffusivity, gathered),
        (field(rows), field(4, rows_slab), field(6, rows), field(LEVELS, 2)),
        scratch=[(5, rows) + tile],
        smem=(0,),
        mib=6,
    )
    before = lax.ppermute(last, "tm", [(q, q + 1) for q in range(count - 1)])
    residual, held = call(
        residual_kernel,
        (before, kept, coef, ab),
        (field(rows), field(4, rows_slab)),
        scratch=[(5, rows) + tile],
    )
    residuals = lax.all_gather(residual, "tm", axis_index_groups=near)
    parts, prefix, added = call(
        spread_kernel,
        (residuals, coef, ab),
        (field(2 * FACTOR - 2, own_rows), field(rows), field(rows_slab)),
        scratch=[(10, rows) + tile],
        mib=6,
    )
    ends = FACTOR - 1
    rank = lax.axis_index("tm")
    wide = lax.div(rank, count // wides)
    place2 = lax.rem(lax.div(rank, FACTOR), FACTOR)

    def message(parts, start):
        return lax.dynamic_slice(parts, (start, 0, 0, 0), (FACTOR,) + parts.shape[1:])

    def inside(value, pairs, block2s):
        return hop(value, [((w, i), (w, j)) for w in block2s for i, j in pairs])

    def direct(parts):
        block2s = range(1)
        summed = inside(parts[ends - 1 :], [(0, 3)], block2s)
        summed = summed + inside(message(parts, jnp.minimum(place2 + 1, 2)), [(0, 2), (1, 3)], block2s)
        summed = summed + inside(message(parts, jnp.minimum(place2, 2)), [(0, 1), (2, 3)], block2s)
        summed = summed + inside(parts[1 : FACTOR + 1], [(1, 2)], block2s)
        return (summed[0], *(parts[ends + i] + summed[1 + i] for i in range(FACTOR - 1)))

    def tree(parts):
        block2s = range(1, wides)

        def early(parts):
            got = inside(parts, [(0, 1)], block2s)
            return tuple(got[i] for i in range(2 * FACTOR - 2))

        none = jnp.zeros_like(parts[0])
        got = lax.cond(place2 <= 1, early, lambda parts: (none,) * (2 * FACTOR - 2), parts)
        pair = parts + jnp.stack(got)

        def late(pair, parts):
            third = inside(parts[ends - 1 :], [(2, 3)], block2s)
            fourth = inside(pair[ends - 1 :], [(1, 3)], block2s)
            next_ = inside(pair[1], [(1, 2)], block2s)
            both = third + fourth
            return (both[0] + next_, *(both[1 + i] for i in range(FACTOR - 1)))

        first2, *got4 = lax.cond(place2 >= 1, late, lambda pair, parts: (none,) * FACTOR, pair, parts)
        return (jnp.where(place2 == 1, got[0], first2), *(pair[ends + i] + got4[i] for i in range(FACTOR - 1)))

    level2, *goals = lax.cond(wide > 0, tree, direct, parts)
    goals = jnp.stack(goals)
    first = hop(goals, [((0, ends), (1, 0))])

    def carry_on(goals, first):
        entry = hop(first, [((1, 0), (1, ends))])

        def between(goals, entry):
            for w in range(1, wides - 1):
                moved = hop(goals[w:] + entry[w:], [((w, ends), (w + 1, ends))])
                entry = jnp.concatenate([entry[:w], entry[w:] + moved])
            size = (1,) + goals.shape[1:]
            return (
                lax.dynamic_slice(goals + entry, (wide, 0, 0, 0), size)[0],
                lax.dynamic_slice(entry, (wide - 1, 0, 0, 0), size)[0],
            )

        leave, own = lax.cond(
            place2 == ends, between, lambda goals, entry: (first[0], first[0]), goals, entry
        )
        for i in range(ends):
            pairs = [((w, ends), (w + 1, i)) for w in range(1, wides - 1)]
            own = own + hop(leave, pairs + ([((1, 0), (1, i))] if i else []))
        return own

    entry = lax.cond(wide > 0, carry_on, lambda goals, first: jnp.zeros_like(goals[0]), goals, first)
    send = call(share_kernel, (level2, entry), field(FACTOR, slabs, 2, own_rows))
    send = send.reshape((FACTOR * slabs, 2, own_rows) + tile)
    received = lax.all_to_all(send, ("tm", "space"), 0, 0, axis_index_groups=square, tiled=True)
    received = received.reshape((FACTOR, slabs, 2, own_rows) + tile)
    return call(
        final_kernel,
        (received, prefix, added, held, coef, ab),
        field(4, rows_slab),
        scratch=[(6, rows) + tile],
    )


def solution(mesh):
    if mesh.shape["tm"] != FACTOR**3:
        raise ValueError("time axis")
    placed = (
        P(("grp", "tm"), "space", None, None),
        P(("grp", "space"), None, None),
        P(None, "space", None, None),
        P("grp"),
    )
    return jax.shard_map(
        local,
        mesh=mesh,
        in_specs=placed,
        out_specs=P(("grp", "tm"), "space", None, None),
        check_vma=False,
    )
```

```python
import jax
import jax.numpy as jnp
from jax import lax
from jax.experimental import pallas as pl
from jax.experimental.pallas import tpu as pltpu
from jax.sharding import PartitionSpec as P

SWEEPS = 4
FACTOR = 4
TIME_UNIT = 0.5
LEVELS = 4
VMEM = pl.BlockSpec(memory_space=pltpu.VMEM)
SMEM = pl.BlockSpec(memory_space=pltpu.SMEM)


def field(*lead):
    return jax.ShapeDtypeStruct(lead + (8, 128), jnp.float32)


def phi(get, put, coef, ab, level):
    rows = coef.shape[1]
    a, b = ab[level, 0], ab[level, 1]
    v = [get(r) for r in range(rows)]
    base = None
    for sweep in range(SWEEPS):
        new = []
        for r in range(rows):
            x = v[r]
            t = coef[2, r] * pltpu.roll(x, x.shape[0] - 1, 0) + coef[3, r] * pltpu.roll(x, 1, 0)
            t = t + (coef[4, r] * pltpu.roll(x, x.shape[1] - 1, 1) + coef[5, r] * pltpu.roll(x, 1, 1))
            if r + 1 < rows:
                t = t + coef[0, r] * v[r + 1]
            if r > 0:
                t = t + coef[1, r] * v[r - 1]
            new.append(a * get(r) + b * t)
        v = new
    for r in range(rows):
        put(r, v[r])


def fill_coefficients(coef, ab, velocity_row, kappa):
    rows = coef.shape[1]
    k = jnp.full(coef.shape[2:], kappa, jnp.float32)
    for r in range(rows):
        for axis in range(3):
            half = 0.5 * velocity_row(axis, r)
            coef[2 * axis, r] = k - half
            coef[2 * axis + 1, r] = k + half
    for level in range(LEVELS):
        h = TIME_UNIT * float(FACTOR) ** level
        a = 1.0 / (1.0 + (6.0 * h) * k)
        ab[level, 0] = a
        ab[level, 1] = h * a


def place():
    rank = lax.axis_index("tm")
    block = rank // FACTOR
    return block // FACTOR, block % FACTOR, rank % FACTOR


def chain_kernel(kappa, gathered, last, kept, coef, ab, fields):
    slab = lax.axis_index("space")
    slabs, chunk = gathered.shape[:2]
    rows_slab = chunk // 8
    rows = slabs * rows_slab
    points = 4

    def row(item, r):
        return gathered[r // rows_slab, item * rows_slab + r % rows_slab]

    fill_coefficients(coef, ab, lambda axis, r: row(points + axis, r), kappa[0])
    first = (lax.axis_index("tm") == 0).astype(jnp.float32)
    for r in range(rows):
        fields[0, r] = row(points + 3, r) * first

    def body(n, carry):
        phi(
            lambda r: fields[n, r],
            lambda r, value: fields.__setitem__((n + 1, r), value + row(n, r)),
            coef, ab, 0,
        )
        return carry

    lax.fori_loop(0, points, body, 0)
    for r in range(rows):
        last[r] = fields[points, r]
    for i in range(points):
        for r in range(rows_slab):
            kept[i, r] = fields[1 + i, slab * rows_slab + r]


def residual_kernel(before, kept, coef, ab, residual, held, fields):
    slab = lax.axis_index("space")
    rows = coef.shape[1]
    rows_slab = kept.shape[1]
    for r in range(rows):
        fields[0, r] = before[r]

    def body(n, carry):
        phi(
            lambda r: fields[n, r],
            lambda r, value: fields.__setitem__((n + 1, r), value),
            coef, ab, 0,
        )
        return carry

    lax.fori_loop(0, 4, body, 0)
    for r in range(rows):
        residual[r] = fields[4, r]
    for r in range(rows_slab):
        for i in range(3):
            held[i, r] = kept[i, r] + fields[1 + i, slab * rows_slab + r]
        held[3, r] = kept[3, r]


def spread_kernel(residuals, coef, ab, parts, prefix, added, fields):
    wide, place2, member = place()
    slab = lax.axis_index("space")
    rows = coef.shape[1]
    rows_slab = added.shape[0]
    own = parts.shape[1]
    for r in range(rows):
        fields[0, r] = jnp.zeros(fields.shape[2:], jnp.float32)
        fields[1, r] = residuals[0, r]

    def step(src, dst, level, add):
        phi(
            lambda r: fields[src, r],
            lambda r, value: fields.__setitem__((dst, r), add(r, value)),
            coef, ab, level,
        )

    def sums(n, carry):
        step(n, n + 1, 1, lambda r, value: value + residuals[n, r])
        return carry

    lax.fori_loop(1, FACTOR, sums, 0)
    total = FACTOR
    z = total + FACTOR - 1 - place2

    def twos(n, carry):
        step(n, n + 1, 2, lambda r, value: value)
        return carry

    lax.fori_loop(total, z, twos, 0)

    def threes(n, carry):
        step(jnp.where(n == 7, z, n), n + 1, 3, lambda r, value: value)
        return carry

    lax.fori_loop(7, 7 + jnp.maximum(FACTOR - 2 - wide, 0), threes, 0)

    def store(slot, source):
        for j in range(own):
            parts[slot, j] = fields[source, slab * rows_slab + member * own + j]

    for later in range(1, FACTOR):
        n = later - 1 - place2
        store(later - 1, jnp.where(n >= 0, total + n, 0))
    for goal in range(FACTOR - 1):
        n = goal - wide
        store(FACTOR - 1 + goal, jnp.where(n < 0, 0, jnp.where(n == 0, z, 7 + n)))
    for r in range(rows):
        prefix[r] = fields[member, r]
    end = member == FACTOR - 1
    for r in range(rows_slab):
        at = slab * rows_slab + r
        added[r] = jnp.where(end, fields[total, at], residuals[member, at])


def share_kernel(level2, entry, send):
    for j in range(entry.shape[0]):
        for a in range(send.shape[0]):
            for s in range(send.shape[1]):
                send[a, s, 0, j] = entry[j]
                send[a, s, 1, j] = level2[j]


def final_kernel(received, prefix, added, held, coef, ab, out, v):
    wide, place2, member = place()
    slab = lax.axis_index("space")
    rows = coef.shape[1]
    rows_slab = out.shape[1]
    own = received.shape[3]

    def item(which, r):
        return received[r % rows_slab // own, r // rows_slab, which, r % own]

    for r in range(rows):
        v[0, r] = item(0, r)
        v[1, r] = item(0, r)
        v[3, r] = item(1, r)

    def apply(dst, src, level):
        phi(lambda r: v[src, r], lambda r, value: v.__setitem__((dst, r), value), coef, ab, level)

    def body(level):
        def run(n, carry):
            apply(1, 1, level)
            return carry

        return run

    lax.fori_loop(0, place2, body(2), 0)
    for r in range(rows):
        entry = v[1, r] + v[3, r]
        v[1, r] = entry
        v[4, r] = entry
    lax.fori_loop(0, member, body(1), 0)
    for r in range(rows):
        v[1, r] = v[1, r] + prefix[r]
        v[5, r] = jnp.zeros(v.shape[2:], jnp.float32)
    end = member == FACTOR - 1
    both = end & (place2 == FACTOR - 1)
    apply(2, jnp.where(both, 0, jnp.where(end, 4, 1)), jnp.where(both, 3, jnp.where(end, 2, 1)))

    def second(n, carry):
        apply(5, 3, 2)
        return carry

    lax.fori_loop(0, jnp.where(both, 1, 0), second, 0)
    for r in range(rows_slab):
        at = slab * rows_slab + r
        out[3, r] = held[3, r] + (v[2, at] + v[5, at] + added[r])

    def last(i, carry):
        apply(1, 1, 0)
        for r in range(rows_slab):
            out[i, r] = held[i, r] + v[1, slab * rows_slab + r]
        return carry

    lax.fori_loop(0, 3, last, 0)


def call(kernel, inputs, outputs, scratch=(), smem=(), mib=4):
    return pl.pallas_call(
        kernel,
        out_shape=outputs,
        in_specs=[SMEM if i in smem else VMEM for i in range(len(inputs))],
        out_specs=jax.tree.map(lambda _: VMEM, outputs),
        scratch_shapes=[pltpu.VMEM(s, jnp.float32) for s in scratch],
        compiler_params=pltpu.CompilerParams(vmem_limit_bytes=mib << 20),
    )(*inputs)


def local(forcing, start_field, velocity, diffusivity):
    count = lax.axis_size("tm")
    slabs = lax.axis_size("space")
    blocks = count // FACTOR
    wides = blocks // FACTOR
    rows_slab = forcing.shape[1]
    rows = rows_slab * slabs
    own_rows = rows_slab // FACTOR
    tile = forcing.shape[2:]

    near = [[FACTOR * m + j for j in range(FACTOR)] for m in range(blocks)]
    square = [[q * slabs + s for q in group for s in range(slabs)] for group in near]

    def hop(value, pairs):
        moves = []
        for source, target in pairs:
            moves += zip(near[source[0] * FACTOR + source[1]], near[target[0] * FACTOR + target[1]])
        return lax.ppermute(value, "tm", moves)

    own = jnp.concatenate([forcing, velocity, start_field[None]], axis=0)
    own = own.reshape((1, 8 * rows_slab) + tile)
    gathered = lax.all_to_all(
        jnp.broadcast_to(own, (slabs,) + own.shape[1:]), "space", 0, 0, tiled=True
    )
    last, kept, coef, ab = call(
        chain_kernel,
        (diffusivity, gathered),
        (field(rows), field(4, rows_slab), field(6, rows), field(LEVELS, 2)),
        scratch=[(5, rows) + tile],
        smem=(0,),
        mib=6,
    )
    before = lax.ppermute(last, "tm", [(q, q + 1) for q in range(count - 1)])
    residual, held = call(
        residual_kernel,
        (before, kept, coef, ab),
        (field(rows), field(4, rows_slab)),
        scratch=[(5, rows) + tile],
    )
    residuals = lax.all_gather(residual, "tm", axis_index_groups=near)
    parts, prefix, added = call(
        spread_kernel,
        (residuals, coef, ab),
        (field(2 * FACTOR - 2, own_rows), field(rows), field(rows_slab)),
        scratch=[(10, rows) + tile],
        mib=6,
    )
    ends = FACTOR - 1
    rank = lax.axis_index("tm")
    wide = lax.div(rank, count // wides)
    place2 = lax.rem(lax.div(rank, FACTOR), FACTOR)

    def message(parts, start):
        return lax.dynamic_slice(parts, (start, 0, 0, 0), (FACTOR,) + parts.shape[1:])

    def inside(value, pairs, block2s):
        return hop(value, [((w, i), (w, j)) for w in block2s for i, j in pairs])

    def direct(parts):
        block2s = range(1)
        summed = inside(parts[ends - 1 :], [(0, 3)], block2s)
        summed = summed + inside(message(parts, jnp.minimum(place2 + 1, 2)), [(0, 2), (1, 3)], block2s)
        summed = summed + inside(message(parts, jnp.minimum(place2, 2)), [(0, 1), (2, 3)], block2s)
        summed = summed + inside(parts[1 : FACTOR + 1], [(1, 2)], block2s)
        return (summed[0], *(parts[ends + i] + summed[1 + i] for i in range(FACTOR - 1)))

    def tree(parts):
        block2s = range(1, wides)

        def early(parts):
            got = inside(parts, [(0, 1)], block2s)
            return tuple(got[i] for i in range(2 * FACTOR - 2))

        none = jnp.zeros_like(parts[0])
        got = lax.cond(place2 <= 1, early, lambda parts: (none,) * (2 * FACTOR - 2), parts)
        pair = parts + jnp.stack(got)

        def late(pair, parts):
            third = inside(parts[ends - 1 :], [(2, 3)], block2s)
            fourth = inside(pair[ends - 1 :], [(1, 3)], block2s)
            next_ = inside(pair[1], [(1, 2)], block2s)
            both = third + fourth
            return (both[0] + next_, *(both[1 + i] for i in range(FACTOR - 1)))

        first2, *got4 = lax.cond(place2 >= 1, late, lambda pair, parts: (none,) * FACTOR, pair, parts)
        return (jnp.where(place2 == 1, got[0], first2), *(pair[ends + i] + got4[i] for i in range(FACTOR - 1)))

    level2, *goals = lax.cond(wide > 0, tree, direct, parts)
    goals = jnp.stack(goals)
    first = hop(goals, [((0, ends), (1, 0))])

    def carry_on(goals, first):
        entry = hop(first, [((1, 0), (1, ends))])

        def between(goals, entry):
            for w in range(1, wides - 1):
                moved = hop(goals[w:] + entry[w:], [((w, ends), (w + 1, ends))])
                entry = jnp.concatenate([entry[:w], entry[w:] + moved])
            size = (1,) + goals.shape[1:]
            return (
                lax.dynamic_slice(goals + entry, (wide, 0, 0, 0), size)[0],
                lax.dynamic_slice(entry, (wide - 1, 0, 0, 0), size)[0],
            )

        leave, own = lax.cond(
            place2 == ends, between, lambda goals, entry: (first[0], first[0]), goals, entry
        )
        for i in range(ends):
            pairs = [((w, ends), (w + 1, i)) for w in range(1, wides - 1)]
            own = own + hop(leave, pairs + ([((1, 0), (1, i))] if i else []))
        return own

    entry = lax.cond(wide > 0, carry_on, lambda goals, first: jnp.zeros_like(goals[0]), goals, first)
    send = call(share_kernel, (level2, entry), field(FACTOR, slabs, 2, own_rows))
    send = send.reshape((FACTOR * slabs, 2, own_rows) + tile)
    received = lax.all_to_all(send, ("tm", "space"), 0, 0, axis_index_groups=square, tiled=True)
    received = received.reshape((FACTOR, slabs, 2, own_rows) + tile)
    return call(
        final_kernel,
        (received, prefix, added, held, coef, ab),
        field(4, rows_slab),
        scratch=[(6, rows) + tile],
    )


def solution(mesh):
    if mesh.shape["tm"] != FACTOR**3:
        raise ValueError("time axis")
    placed = (
        P(("grp", "tm"), "space", None, None),
        P(("grp", "space"), None, None),
        P(None, "space", None, None),
        P("grp"),
    )
    return jax.shard_map(
        local,
        mesh=mesh,
        in_specs=placed,
        out_specs=P(("grp", "tm"), "space", None, None),
        check_vma=False,
    )
```
